32 devices in a mesh: slab: 32 (over z, y, x, core).
Axes of the slice: x: 2, y: 2, z: 4, core: 2. Of those that a mesh axis runs over, the one named last changes fastest.
Arguments:
- points: float32 [4, 128, 128, 64], P(None, 'slab'), may hold values from -6 to 6
- offsets_x: int32 [256], replicated, may hold values from 0 to 124, as said below
- coeffs_x: float32 [4, 256], replicated, may hold values from 0.1 to 1
- offsets_y: int32 [256], replicated, may hold values from 0 to 124, as said below
- coeffs_y: float32 [4, 256], replicated, may hold values from 0.1 to 1
- offsets_z: int32 [128], replicated, may hold values from 0 to 60, as said below
- coeffs_z: float32 [4, 128], replicated, may hold values from 0.1 to 1
Outputs:
- refined: float32 [4, 256, 256, 128], P(None, None, 'slab')
The draws below stay inside these ranges and needn't reach their ends.
Inputs may be any that keep to these rules, and one draw needn't show every extreme that they name: offsets_x[i] lies between i // 2 - 2 and i // 2, clipped to 0 .. 124. offsets_y[i] lies between i // 2 - 2 and i // 2, clipped to 0 .. 124. offsets_z[i] lies between i // 2 - 2 and i // 2, clipped to 0 .. 60.
All inputs are finite; a program needn't handle non-finite values.
Results may differ from the reference program's by a relative error of at most 0.000073.
Values sent between devices are 32-bit elements; how exact they have to be, the bound alone decides.
A program may use at most 64 MiB of HBM per device.

```python
import math
import jax
import jax.numpy as jnp

NY = 128
NZ = 64
NX = 128
MX = 256
MY = 256
MZ = 128


def band_offsets(key, count):
    rows = jnp.arange(2 * count, dtype=jnp.int32)
    jitter = jax.random.randint(key, (2 * count,), 0, 3, dtype=jnp.int32)
    return jnp.clip(rows // 2 - 2 + jitter, 0, count - 4).astype(jnp.int32)


def draw_offsets_x(key, part):
    return band_offsets(jax.random.fold_in(key, 11), NX)


def draw_offsets_y(key, part):
    return band_offsets(jax.random.fold_in(key, 12), NY)


def draw_offsets_z(key, part):
    return band_offsets(jax.random.fold_in(key, 13), NZ)


def steps_of(rng, dims, split, least, largest):
    gain = 1.0
    for dim, shards_of in split:
        steps = jax.random.uniform(jax.random.fold_in(jax.random.fold_in(rng, 6), dim), (shards_of,), jnp.float32, least / len(split), largest / len(split))
        gain = gain * jnp.repeat(jnp.exp(steps), dims[dim] // shards_of).reshape((-1,) + (1,) * (len(dims) - 1 - dim))
    return gain


def normal_values(own_key, extent, spread, reach, pieces=(), kind=jnp.bfloat16):
    entries = spread * jax.random.normal(own_key, extent, jnp.float32)
    if pieces:
        entries = entries * steps_of(own_key, extent, pieces, -0.22, 0.18)
    return jnp.clip(entries, -reach, reach).astype(kind)


def setup_inputs(seed: int = 0) -> dict:
    keys = jax.random.split(jax.random.key(seed), 8)
    points = normal_values(keys[0], (4, NX, NY, NZ), 1.0, 6.0, ((1, 32),), jnp.float32)
    offsets_x = draw_offsets_x(jax.random.fold_in(keys[7], 71), 0)
    coeffs_x = jnp.clip(jnp.exp(jax.random.uniform(keys[2], (4, MX), jnp.float32, math.log(0.1), math.log(1.0))), 0.1, 1.0)
    offsets_y = draw_offsets_y(jax.random.fold_in(keys[7], 71), 0)
    coeffs_y = jnp.clip(jnp.exp(jax.random.uniform(keys[4], (4, MY), jnp.float32, math.log(0.1), math.log(1.0))), 0.1, 1.0)
    offsets_z = draw_offsets_z(jax.random.fold_in(keys[7], 71), 0)
    coeffs_z = jnp.clip(jnp.exp(jax.random.uniform(keys[6], (4, MZ), jnp.float32, math.log(0.1), math.log(1.0))), 0.1, 1.0)
    return {"points": points, "offsets_x": offsets_x, "coeffs_x": coeffs_x, "offsets_y": offsets_y, "coeffs_y": coeffs_y, "offsets_z": offsets_z, "coeffs_z": coeffs_z}


def refine(grid, offsets, coeffs, axis):
    weights = coeffs / jnp.sum(coeffs, axis=0, keepdims=True)
    shape = [1] * grid.ndim
    shape[axis] = -1
    total = None
    for k in range(4):
        picked = jnp.take(grid, (offsets + k).astype(jnp.int32), axis=axis)
        term = picked * weights[k].reshape(shape)
        total = term if total is None else total + term
    return total


def reference(points, offsets_x, coeffs_x, offsets_y, coeffs_y, offsets_z, coeffs_z):
    grid = refine(points, offsets_z, coeffs_z, 3)
    grid = refine(grid, offsets_y, coeffs_y, 2)
    return refine(grid, offsets_x, coeffs_x, 1)
```

```python
import functools

import jax
import jax.numpy as jnp
from jax import lax
from jax.experimental import pallas as pl
from jax.experimental.pallas import tpu as pltpu
from jax.sharding import PartitionSpec as P

MESH = pl.DeviceIdType.MESH
BAND = 4
REACH = BAND + 1
SPAN = BAND + 2
BELOW, ABOVE = 2, 3
PLANES = 4
GROUP = 8
VMEM_MOST = 67043328


def flip(a, k, chips):
    out = 0
    bit = 1
    while bit < chips:
        a_bit, k_bit = lax.rem(lax.div(a, bit), 2), (k // bit) % 2
        out = out + (a_bit + k_bit - 2 * a_bit * k_bit) * bit
        bit *= 2
    return out


def span_of(me, jl, ny, j):
    return jnp.clip((me * jl + j) // 2 - 2, 0, ny - SPAN)


def make_weights(dims, me, span_base, oy_ref, cy_ref, oz_ref, cz_ref, cx_ref, wx_ref, wy, rz, rz_lo):
    n, comps, xl, ny, nz, jl, mz = dims
    pairs, lanes = wy.shape[1], wy.shape[2]
    fold = lanes // nz
    wx_ref[...] = cx_ref[...] / jnp.sum(cx_ref[...], axis=0, keepdims=True)
    wz = cz_ref[...] / jnp.sum(cz_ref[...], axis=0, keepdims=True)
    at = lax.broadcasted_iota(jnp.int32, (nz, mz), 0)
    first = jnp.broadcast_to(oz_ref[...], (nz, mz))
    band = jnp.zeros((nz, mz), jnp.float32)
    for k in range(BAND):
        band = band + jnp.where(at == first + k, jnp.broadcast_to(wz[k : k + 1], (nz, mz)), 0.0)
    high = band.astype(jnp.bfloat16)
    low = (band - high.astype(jnp.float32)).astype(jnp.bfloat16)
    rz[...] = jnp.zeros_like(rz)
    rz_lo[...] = jnp.zeros_like(rz_lo)
    for f in range(fold):
        rz[f * nz : (f + 1) * nz, f * mz : (f + 1) * mz] = high
        rz[lanes + f * nz : lanes + (f + 1) * nz, f * mz : (f + 1) * mz] = high
        rz_lo[f * nz : (f + 1) * nz, f * mz : (f + 1) * mz] = low
    for j in range(jl):
        coeffs = [jnp.full((pairs, lanes), cy_ref[k, me * jl + j]) for k in range(BAND)]
        total = coeffs[0] + coeffs[1] + coeffs[2] + coeffs[3]
        coeffs = [c / total for c in coeffs]
        skip = jnp.full((pairs, lanes), oy_ref[me * jl + j] - span_base(j))
        for m in range(SPAN):
            weight = jnp.zeros((pairs, lanes), jnp.float32)
            for k in range(max(0, m - SPAN + BAND), min(BAND, m + 1)):
                weight = jnp.where(skip == m - k, coeffs[k], weight)
            wy[j * SPAN + m] = weight


def refine_y(jl, pairs, span_base, wy, mixed, place, load, base):
    for j in range(jl):
        row = span_base(j) - base
        acc = wy[j * SPAN] * load(row)
        for m in range(1, SPAN):
            acc = acc + wy[j * SPAN + m] * load(row + m)
        mixed[pl.ds(place * pairs * jl + j, pairs, stride=jl), :] = acc


def refine_z(dims, pairs, mixed, rz, rz_lo, grid_ref, devices):
    n, comps, xl, ny, nz, jl, mz = dims
    fold = mixed.shape[1] // nz
    rows = pairs * jl * len(devices)
    x = mixed[:rows]
    hi = x.astype(jnp.bfloat16)
    lo = (x - hi.astype(jnp.float32)).astype(jnp.bfloat16)
    both = jnp.concatenate([hi, lo], axis=1)
    res = jnp.dot(both, rz[...], preferred_element_type=jnp.float32)
    res = res + jnp.dot(hi, rz_lo[...], preferred_element_type=jnp.float32)
    per = pairs // comps
    for q, device in enumerate(devices):
        for p in range(pairs):
            for f in range(fold):
                spot = (p // per, device * xl + (p % per) * fold + f)
                top = (q * pairs + p) * jl
                grid_ref[spot] = res[top : top + jl, f * mz : (f + 1) * mz]


def exchange(
    dims,
    points_ref, oy_ref, cy_ref, oz_ref, cz_ref, cx_ref,
    grid_ref, wx_ref,
    send, direct, passed, wy, rz, rz_lo, mixed,
    send_sem, recv_sem, pass_send_sem, pass_recv_sem,
):
    n, comps, xl, ny, nz, jl, mz = dims
    chips = n // 2
    pairs, lanes = points_ref.shape[0], points_ref.shape[1]
    cl = jl // 2
    wide, narrow = 2 * cl + REACH, cl + REACH
    me = lax.axis_index("slab")
    chip, core = me // 2, me % 2
    partner = chip * 2 + 1 - core

    def wide_base(c):
        return jnp.clip(c * 2 * cl - 2, 0, ny - wide)

    def narrow_base(d):
        return jnp.clip(d * cl - 2, 0, ny - narrow)

    span_base = functools.partial(span_of, me, jl, ny)

    rows_of_y = send.reshape(ny, pairs, lanes)

    barrier = pltpu.get_barrier_semaphore()
    pl.semaphore_signal(barrier, inc=1, device_id=(partner,), device_id_type=MESH)

    @pl.loop(1, chips)
    def _(k):
        other = flip(chip, k, chips) * 2 + core
        pl.semaphore_signal(barrier, inc=1, device_id=(other,), device_id_type=MESH)

    for p in range(pairs):
        send[pl.ds(p, ny, stride=pairs), :] = points_ref[p].T

    pl.semaphore_wait(barrier, chips)

    def out_copy(k):
        target = flip(chip, k, chips)
        return pltpu.make_async_remote_copy(
            src_ref=rows_of_y.at[pl.ds(wide_base(target), wide)],
            dst_ref=direct.at[k],
            send_sem=send_sem.at[k],
            recv_sem=recv_sem.at[k],
            device_id=(target * 2 + core,),
            device_id_type=MESH,
        )

    def pass_copy(k):
        skip = narrow_base(partner) - wide_base(chip)
        return pltpu.make_async_remote_copy(
            src_ref=direct.at[k, pl.ds(skip, narrow)],
            dst_ref=passed.at[k],
            send_sem=pass_send_sem.at[k],
            recv_sem=pass_recv_sem.at[k],
            device_id=(partner,),
            device_id_type=MESH,
        )

    @pl.loop(1, chips)
    def _(k):
        out_copy(k).start()

    own = pl.ds(wide_base(chip), wide)
    stay = pltpu.make_async_copy(rows_of_y.at[own], direct.at[0], recv_sem.at[0])
    stay.start()

    make_weights(dims, me, span_base, oy_ref, cy_ref, oz_ref, cz_ref, cx_ref, wx_ref, wy, rz, rz_lo)

    def from_direct(place, k):
        refine_y(
            jl, pairs, span_base, wy, mixed, place,
            lambda row: direct[k, row],
            wide_base(chip),
        )
        return flip(chip, k, chips) * 2 + core

    def from_passed(place, k):
        refine_y(
            jl, pairs, span_base, wy, mixed, place,
            lambda row: passed[k, row],
            narrow_base(me),
        )
        return flip(chip, k, chips) * 2 + 1 - core

    stay.wait()
    pass_copy(0).start()
    refine_z(dims, pairs, mixed, rz, rz_lo, grid_ref, [from_direct(0, 0)])

    @pl.loop(1, chips)
    def _(k):
        out_copy(k).wait_recv()
        pass_copy(k).start()
        one = from_direct(0, k)
        pass_copy(k - 1).wait_recv()
        two = from_passed(1, k - 1)
        refine_z(dims, pairs, mixed, rz, rz_lo, grid_ref, [one, two])

    pass_copy(chips - 1).wait_recv()
    refine_z(dims, pairs, mixed, rz, rz_lo, grid_ref, [from_passed(0, chips - 1)])

    @pl.loop(1, chips)
    def _(k):
        out_copy(k).wait_send()

    @pl.loop(0, chips)
    def _(k):
        pass_copy(k).wait_send()


def relay(
    dims,
    points_hbm, oy_hbm, cy_hbm, oz_hbm, cz_hbm, cx_hbm, ox_hbm,
    block_ref,
    slab, send, direct, passed, wy, rz, rz_lo, mixed,
    oy_ref, cy_ref, oz_ref, cz_ref, cx_ref,
    grid_ref, ox_ref, wx_ref, wx_scalars,
    load_sem, small_sem, out_sem, hand_sem, pass_sem,
    whole_recv, low_recv, high_recv, middle_recv, pass_recv,
    flags, partner_flag,
):
    n, comps, xl, ny, nz, jl, mz = dims
    chips = n // 2
    plane = chips // PLANES
    pairs, lanes = slab.shape[0], slab.shape[1]
    own, half = jl, jl // 2
    wide, narrow = own + REACH, half + REACH
    whole, low, high = pl.ds(0, wide), pl.ds(0, REACH), pl.ds(own, REACH)
    middle = pl.ds(REACH, own - REACH)
    me = lax.axis_index("slab")
    chip, core = lax.div(me, 2), lax.rem(me, 2)
    partner = chip * 2 + 1 - core
    here, level = lax.rem(chip, plane), lax.div(chip, plane)
    rows_of_y = send.reshape(ny + REACH, pairs, lanes)
    any_rows = direct.reshape(PLANES * plane * wide, pairs, lanes)
    span_base = functools.partial(span_of, me, jl, ny)
    around = [flip(here, d, plane) for d in range(plane)]

    loads = [pltpu.make_async_copy(points_hbm.at[p], slab.at[p], load_sem.at[p]) for p in range(pairs)]
    for load in loads:
        load.start()

    barrier = pltpu.get_barrier_semaphore()

    def greet(semaphore, device):
        pl.semaphore_signal(semaphore, inc=1, device_id=(device,), device_id_type=MESH)

    def device_of(z, q):
        return (z * plane + q) * 2 + core

    side = [lax.rem(here, 2), lax.div(here, 2)]
    above = [None, side[0] == 0, side[1] == 0, side[0] + side[1] == 0]
    below = [None, side[0] == 1, side[1] == 1, side[0] + side[1] == 2]
    missing = [None, side[0] == 0, side[1] == 0, side[0] + side[1] < 2]

    @pl.when(core == 0)
    def _():
        greet(barrier, partner)

    for d in range(plane):
        def hail(d=d):
            @pl.loop(level + (d == 0), PLANES)
            def _(z):
                greet(barrier, device_of(z, around[d]))

        hail() if d == 0 else pl.when(above[d])(hail)

    smalls = [
        pltpu.make_async_copy(src, dst, small_sem.at[i])
        for i, (src, dst) in enumerate(
            [(oy_hbm, oy_ref), (cy_hbm, cy_ref), (oz_hbm, oz_ref), (cz_hbm, cz_ref), (cx_hbm, cx_ref), (ox_hbm, ox_ref)]
        )
    ]
    for small in smalls:
        small.start()

    @pl.when(me > 0)
    def _():
        pl.semaphore_wait(barrier, (level + 1) * (1 + side[0]) * (1 + side[1]) - 1 + core)

    for d in range(plane):
        def answer(d=d):
            @pl.loop(0, level + (d != 0))
            def _(z):
                greet(flags.at[chip], device_of(z, around[d]))

        answer() if d == 0 else pl.when(below[d])(answer)

    def introduce(za, qa, zb, qb):
        greet(flags.at[zb * plane + qb], device_of(za, qa))
        greet(flags.at[za * plane + qa], device_of(zb, qb))

    for q in range(1, plane):
        @pl.when(here == q)
        def _():
            if q == plane - 1:
                introduce(level, 1, level, 2)

            @pl.loop(0, level)
            def _(z):
                for low_q in range(plane):
                    for high_q in range(plane):
                        if low_q | high_q == q and high_q != q:
                            if low_q & ~high_q:
                                introduce(z, low_q, level, high_q)

    @pl.when(core == 1)
    def _():
        greet(partner_flag, partner)

    for edge in (pl.ds(0, BELOW), pl.ds(BELOW + ny, ABOVE)):
        rows_of_y[edge] = jnp.zeros((edge.size, pairs, lanes), jnp.float32)
    for p in range(pairs):
        loads[p].wait()
        send[pl.ds(BELOW * pairs + p, ny, stride=pairs), :] = slab[p].T

    def remote(src, dst, send_sem, recv_sem, device):
        return pltpu.make_async_remote_copy(
            src_ref=src, dst_ref=dst, send_sem=send_sem, recv_sem=recv_sem,
            device_id=(device,), device_id_type=MESH,
        )

    def await_recv(ref, semaphore):
        remote(ref, ref, out_sem, semaphore, partner).wait_recv()

    def await_send(count, semaphore):
        rows = any_rows.at[pl.ds(0, count)]
        remote(rows, rows, semaphore, pass_recv.at[0], partner).wait_send()

    def put(z, q, rows, semaphores):
        remote(
            rows_of_y.at[pl.ds((z * plane + q) * own + rows.start, rows.size)],
            direct.at[level, here, rows], out_sem, semaphores.at[level],
            (z * plane + q) * 2 + core,
        ).start()

    def ask(mine, z, d):
        def wait():
            pl.semaphore_wait(flags.at[z * plane + around[d]], 1)

        if z > mine:
            wait()
        elif d:
            pl.when(missing[d])(wait)

    def send_whole(mine, targets):
        for d in range(plane):
            for z in targets:
                ask(mine, z, d)
                put(z, around[d], whole, whole_recv)

    def send_ends(mine, targets):
        for d in range(plane):
            for z in targets:
                ask(mine, z, d)
                put(z, around[d], low, low_recv)

                @pl.when(around[d] == plane - 1)
                def _():
                    put(z, around[d], high, high_recv)

    def send_middle(mine, targets):
        for d in range(plane)[::-1]:
            for z in targets:
                put(z, around[d], middle, middle_recv)

    def send_plane(mine, targets):
        for d in range(1, plane):
            ask(mine, mine, d)
            put(mine, around[d], whole, whole_recv)

    def pass_copy(z):
        return remote(
            direct.at[z, :, pl.ds((1 - core) * half, narrow)], passed.at[z],
            pass_sem, pass_recv.at[z], partner,
        )

    def refine(blocks, base, devices):
        for j in range(jl):
            row = span_base(j) - base
            sums = [None] * len(blocks)
            for m in range(SPAN):
                weight = wy[j * SPAN + m]
                for i, block in enumerate(blocks):
                    term = weight * block[row + m]
                    sums[i] = term if m == 0 else sums[i] + term
            for i, total in enumerate(sums):
                mixed[pl.ds(i * pairs * jl + j, pairs, stride=jl), :] = total
        refine_z(dims, pairs, mixed, rz, rz_lo, grid_ref, devices)

    def take_whole(z):
        await_recv(direct.at[z], whole_recv.at[z])
        pass_copy(z).start()

    def take_plane(z):
        await_recv(direct.at[z, pl.ds(0, plane - 1)], whole_recv.at[z])
        pass_copy(z).start()

    def take_low(z):
        await_recv(direct.at[z, :, low], low_recv.at[z])

        @pl.when(here > 0)
        def _():
            remote(
                direct.at[z, :, low], direct.at[z, :, high], hand_sem, high_recv.at[z], (chip - 1) * 2 + core
            ).start()

    def take_middle(z):
        await_recv(direct.at[z, :, high], high_recv.at[z])
        await_recv(direct.at[z, :, middle], middle_recv.at[z])
        pass_copy(z).start()

    def near(z):
        refine(
            [direct.at[z, q] for q in range(plane)], chip * own - BELOW,
            [(z * plane + q) * 2 + core for q in range(plane)],
        )

    def far(z):
        pass_copy(z).wait_recv()
        refine(
            [passed.at[z, q] for q in range(plane)], me * half - BELOW,
            [(z * plane + q) * 2 + 1 - core for q in range(plane)],
        )

    mx = wx_ref.shape[1]
    part, margin = mx // PLANES, GROUP

    def across(*zs):
        first, last = min(zs), max(zs) + 1
        start = first * part
        stop = last * part
        if len(zs) > 1:
            start += margin * (first > 0)
            stop -= margin * (last < PLANES)
        elif first in (0, PLANES - 1):
            start += margin * (first > 0)
            stop -= margin * (last < PLANES)
        else:
            start -= margin
            stop += margin
        refine_rows(start, stop)

    def refine_rows(start, stop):
        @pl.loop(start // GROUP, stop // GROUP)
        def _(g):
            done = []
            for r in range(GROUP):
                i = g * GROUP + r
                first = ox_ref[i]
                weights = [wx_scalars[k, i] for k in range(BAND)]
                for c in range(comps):
                    acc = weights[0] * grid_ref[c, first]
                    for k in range(1, BAND):
                        acc = acc + weights[k] * grid_ref[c, first + k]
                    done.append((c, i, acc))
            for c, i, acc in done:
                block_ref[c, i] = acc

    acts = {
        "W": send_whole, "E": send_ends, "M": send_middle, "P": send_plane,
        "w": take_whole, "p": take_plane, "e": take_low, "m": take_middle, "n": near, "f": far, "x": across,
    }
    sends = [
        ["P0", "W1", "E2", "E3", "M2", "M3"],
        ["W0", "P1", "E2", "E3", "M2", "M3"],
        ["E01", "P2", "W3", "M0", "M1"],
        ["E01", "W2", "P3", "M0", "M1"],
    ]
    takes = [
        ["p0", "n0", "e3", "e2", "f0", "w1", "n1", "f1", "x01", "m3", "n3", "f3", "x3", "m2", "n2", "f2", "x2"],
        ["p1", "n1", "w0", "n0", "f1", "e3", "e2", "f0", "x01", "m3", "n3", "f3", "x3", "m2", "n2", "f2", "x2"],
        ["p2", "n2", "e1", "e0", "f2", "w3", "n3", "f3", "x23", "m0", "n0", "f0", "x0", "m1", "n1", "f1", "x1"],
        ["p3", "n3", "w2", "n2", "f3", "e0", "e1", "f2", "x23", "m0", "n0", "f0", "x0", "m1", "n1", "f1", "x1"],
    ]

    for z, plan in enumerate(sends):

        @pl.when(level == z)
        def _():
            for step in plan:
                acts[step[0]](z, [int(target) for target in step[1:]])

    direct[level, here] = rows_of_y[pl.ds(chip * own, wide)]

    @pl.when(core == 0)
    def _():
        pl.semaphore_wait(partner_flag, 1)

    for small in smalls:
        small.wait()
    make_weights(dims, me, span_base, oy_ref, cy_ref, oz_ref, cz_ref, cx_ref, wx_ref, wy, rz, rz_lo)
    scalars = pltpu.make_async_copy(wx_ref, wx_scalars, small_sem.at[0])
    scalars.start()
    scalars.wait()

    for z, plan in enumerate(takes):

        @pl.when(level == z)
        def _():
            for step in plan:
                acts[step[0]](*[int(target) for target in step[1:]])

    await_send(2 * (plane * own + REACH) + (2 * plane - 1) * wide, out_sem)

    @pl.when(here > 0)
    def _():
        await_send(2 * plane * REACH, hand_sem)

    await_send(PLANES * plane * narrow, pass_sem)


def refine_x(steps, ox_ref, wx_ref, grid_ref, out_ref, block, sems):
    comps, mx = block.shape[0], block.shape[1]
    rows = mx // steps

    def put(s):
        part = pl.ds(pl.multiple_of(s * rows, rows), rows)
        return pltpu.make_async_copy(block.at[:, part], out_ref.at[:, part], sems.at[s])

    @pl.loop(0, steps)
    def _(s):
        @pl.loop(0, rows // GROUP)
        def _(g):
            done = []
            for q in range(GROUP):
                i = s * rows + g * GROUP + q
                first = ox_ref[i]
                weights = [wx_ref[k, i] for k in range(BAND)]
                for c in range(comps):
                    acc = weights[0] * grid_ref[c, first]
                    for k in range(1, BAND):
                        acc = acc + weights[k] * grid_ref[c, first + k]
                    done.append((c, i, acc))
            for c, i, acc in done:
                block[c, i] = acc

        put(s).start()

    @pl.loop(0, steps)
    def _(s):
        put(s).wait()


def store(block_ref, out_ref, sems):
    copies = [pltpu.make_async_copy(block_ref.at[c], out_ref.at[c], sems.at[c]) for c in range(block_ref.shape[0])]
    for copy in copies:
        copy.start()
    for copy in copies:
        copy.wait()


def solution(mesh):
    n = mesh.shape["slab"]
    vmem = pl.BlockSpec(memory_space=pltpu.VMEM)
    smem = pl.BlockSpec(memory_space=pltpu.SMEM)

    def body(points, offsets_x, coeffs_x, offsets_y, coeffs_y, offsets_z, coeffs_z):
        comps, xl, ny, nz = points.shape
        nx = xl * n
        mx, my, mz = offsets_x.shape[0], offsets_y.shape[0], offsets_z.shape[0]
        jl = my // n
        fold = 128 // nz
        pairs = comps * xl // fold
        lanes = fold * nz
        chips = n // 2
        cl = jl // 2
        wide, narrow = 2 * cl + REACH, cl + REACH
        slab = jnp.transpose(points, (0, 1, 3, 2)).reshape(pairs, lanes, ny)
        f32, bf16 = jnp.float32, jnp.bfloat16
        f32_rows = lambda *shape: pltpu.VMEM((*shape, pairs, lanes), f32)
        shared = [
            pltpu.VMEM((jl * SPAN, pairs, lanes), f32),
            pltpu.VMEM((2 * lanes, fold * mz), bf16),
            pltpu.VMEM((lanes, fold * mz), bf16),
            pltpu.VMEM((4 * pairs * jl, lanes), f32),
        ]
        semaphores = lambda *shape: pltpu.SemaphoreType.DMA(shape)
        if jl > REACH and chips == PLANES * PLANES and my == 2 * ny and mx % (PLANES * GROUP) == 0:
            plane = chips // PLANES
            limit = VMEM_MOST - 4 * comps * mx * jl * mz
            hbm = pl.BlockSpec(memory_space=pltpu.HBM)
            block = pl.pallas_call(
                functools.partial(relay, (n, comps, xl, ny, nz, jl, mz)),
                out_shape=pltpu.VMEM((comps, mx, jl, mz), f32),
                in_specs=[hbm] * 7,
                out_specs=vmem,
                scratch_shapes=[
                    pltpu.VMEM((pairs, lanes, ny), f32),
                    pltpu.VMEM(((ny + REACH) * pairs, lanes), f32),
                    f32_rows(PLANES, plane, jl + REACH),
                    f32_rows(PLANES, plane, cl + REACH),
                    *shared,
                    pltpu.SMEM((my,), jnp.int32),
                    pltpu.SMEM((BAND, my), f32),
                    pltpu.VMEM((1, mz), jnp.int32),
                    pltpu.VMEM((BAND, mz), f32),
                    pltpu.VMEM((BAND, mx), f32),
                    pltpu.VMEM((comps, nx, jl, mz), f32),
                    pltpu.SMEM((mx,), jnp.int32),
                    pltpu.VMEM((BAND, mx), f32),
                    pltpu.SMEM((BAND, mx), f32),
                    semaphores(pairs),
                    semaphores(6),
                    *[pltpu.SemaphoreType.DMA] * 3,
                    *[semaphores(PLANES)] * 5,
                    pltpu.SemaphoreType.REGULAR((chips,)),
                    pltpu.SemaphoreType.REGULAR,
                ],
                compiler_params=pltpu.CompilerParams(
                    collective_id=0, has_side_effects=True, vmem_limit_bytes=limit
                ),
                name="relay",
            )(slab, offsets_y, coeffs_y, offsets_z.reshape(1, mz), coeffs_z, coeffs_x, offsets_x)
            return pl.pallas_call(
                store,
                out_shape=jax.ShapeDtypeStruct((comps, mx, jl, mz), f32),
                in_specs=[vmem],
                out_specs=pl.BlockSpec(memory_space=pltpu.HBM),
                scratch_shapes=[semaphores(comps)],
                compiler_params=pltpu.CompilerParams(vmem_limit_bytes=limit),
                name="store",
            )(pltpu.with_memory_space_constraint(block, pltpu.VMEM))
        grid, wx = pl.pallas_call(
            functools.partial(exchange, (n, comps, xl, ny, nz, jl, mz)),
            out_shape=(
                pltpu.VMEM((comps, nx, jl, mz), f32),
                jax.ShapeDtypeStruct((BAND, mx), f32),
            ),
            in_specs=[vmem, smem, smem, vmem, vmem, vmem],
            out_specs=(vmem, vmem),
            scratch_shapes=[
                pltpu.VMEM((ny * pairs, lanes), f32),
                f32_rows(chips, wide),
                f32_rows(chips, narrow),
                *shared,
                *[semaphores(chips)] * 4,
            ],
            compiler_params=pltpu.CompilerParams(collective_id=0, has_side_effects=True),
            name="exchange",
        )(slab, offsets_y, coeffs_y, offsets_z.reshape(1, mz), coeffs_z, coeffs_x)
        steps = 8
        return pl.pallas_call(
            functools.partial(refine_x, steps),
            out_shape=jax.ShapeDtypeStruct((comps, mx, jl, mz), f32),
            in_specs=[smem, smem, vmem],
            out_specs=pl.BlockSpec(memory_space=pltpu.HBM),
            scratch_shapes=[
                pltpu.VMEM((comps, mx, jl, mz), f32),
                pltpu.SemaphoreType.DMA((steps,)),
            ],
            name="refine_x",
        )(offsets_x, wx, pltpu.with_memory_space_constraint(grid, pltpu.VMEM))

    return jax.shard_map(
        body,
        mesh=mesh,
        in_specs=(P(None, "slab", None, None), P(), P(), P(), P(), P(), P()),
        out_specs=P(None, None, "slab", None),
        check_vma=False,
    )
```

```python
import functools

import jax
import jax.numpy as jnp
from jax import lax
from jax.experimental import pallas as pl
from jax.experimental.pallas import tpu as pltpu
from jax.sharding import PartitionSpec as P

MESH = pl.DeviceIdType.MESH
BAND = 4
REACH = BAND + 1
SPAN = BAND + 2
BELOW, ABOVE = 2, 3
PLANES = 4
GROUP = 8
VMEM_MOST = 67043328


def flip(a, k, chips):
    out = 0
    bit = 1
    while bit < chips:
        a_bit, k_bit = lax.rem(lax.div(a, bit), 2), (k // bit) % 2
        out = out + (a_bit + k_bit - 2 * a_bit * k_bit) * bit
        bit *= 2
    return out


def span_of(me, jl, ny, j):
    return jnp.clip((me * jl + j) // 2 - 2, 0, ny - SPAN)


def make_weights(dims, me, span_base, oy_ref, cy_ref, oz_ref, cz_ref, cx_ref, wx_ref, wy, rz, rz_lo):
    n, comps, xl, ny, nz, jl, mz = dims
    pairs, lanes = wy.shape[1], wy.shape[2]
    fold = lanes // nz
    wx_ref[...] = cx_ref[...] / jnp.sum(cx_ref[...], axis=0, keepdims=True)
    wz = cz_ref[...] / jnp.sum(cz_ref[...], axis=0, keepdims=True)
    at = lax.broadcasted_iota(jnp.int32, (nz, mz), 0)
    first = jnp.broadcast_to(oz_ref[...], (nz, mz))
    band = jnp.zeros((nz, mz), jnp.float32)
    for k in range(BAND):
        band = band + jnp.where(at == first + k, jnp.broadcast_to(wz[k : k + 1], (nz, mz)), 0.0)
    high = band.astype(jnp.bfloat16)
    low = (band - high.astype(jnp.float32)).astype(jnp.bfloat16)
    rz[...] = jnp.zeros_like(rz)
    rz_lo[...] = jnp.zeros_like(rz_lo)
    for f in range(fold):
        rz[f * nz : (f + 1) * nz, f * mz : (f + 1) * mz] = high
        rz[lanes + f * nz : lanes + (f + 1) * nz, f * mz : (f + 1) * mz] = high
        rz_lo[f * nz : (f + 1) * nz, f * mz : (f + 1) * mz] = low
    for j in range(jl):
        coeffs = [jnp.full((pairs, lanes), cy_ref[k, me * jl + j]) for k in range(BAND)]
        total = coeffs[0] + coeffs[1] + coeffs[2] + coeffs[3]
        coeffs = [c / total for c in coeffs]
        skip = jnp.full((pairs, lanes), oy_ref[me * jl + j] - span_base(j))
        for m in range(SPAN):
            weight = jnp.zeros((pairs, lanes), jnp.float32)
            for k in range(max(0, m - SPAN + BAND), min(BAND, m + 1)):
                weight = jnp.where(skip == m - k, coeffs[k], weight)
            wy[j * SPAN + m] = weight


def refine_y(jl, pairs, span_base, wy, mixed, place, load, base):
    for j in range(jl):
        row = span_base(j) - base
        acc = wy[j * SPAN] * load(row)
        for m in range(1, SPAN):
            acc = acc + wy[j * SPAN + m] * load(row + m)
        mixed[pl.ds(place * pairs * jl + j, pairs, stride=jl), :] = acc


def refine_z(dims, pairs, mixed, rz, rz_lo, grid_ref, devices):
    n, comps, xl, ny, nz, jl, mz = dims
    fold = mixed.shape[1] // nz
    rows = pairs * jl * len(devices)
    x = mixed[:rows]
    hi = x.astype(jnp.bfloat16)
    lo = (x - hi.astype(jnp.float32)).astype(jnp.bfloat16)
    both = jnp.concatenate([hi, lo], axis=1)
    res = jnp.dot(both, rz[...], preferred_element_type=jnp.float32)
    res = res + jnp.dot(hi, rz_lo[...], preferred_element_type=jnp.float32)
    per = pairs // comps
    for q, device in enumerate(devices):
        for p in range(pairs):
            for f in range(fold):
                spot = (p // per, device * xl + (p % per) * fold + f)
                top = (q * pairs + p) * jl
                grid_ref[spot] = res[top : top + jl, f * mz : (f + 1) * mz]


def exchange(
    dims,
    points_ref, oy_ref, cy_ref, oz_ref, cz_ref, cx_ref,
    grid_ref, wx_ref,
    send, direct, passed, wy, rz, rz_lo, mixed,
    send_sem, recv_sem, pass_send_sem, pass_recv_sem,
):
    n, comps, xl, ny, nz, jl, mz = dims
    chips = n // 2
    pairs, lanes = points_ref.shape[0], points_ref.shape[1]
    cl = jl // 2
    wide, narrow = 2 * cl + REACH, cl + REACH
    me = lax.axis_index("slab")
    chip, core = me // 2, me % 2
    partner = chip * 2 + 1 - core

    def wide_base(c):
        return jnp.clip(c * 2 * cl - 2, 0, ny - wide)

    def narrow_base(d):
        return jnp.clip(d * cl - 2, 0, ny - narrow)

    span_base = functools.partial(span_of, me, jl, ny)

    rows_of_y = send.reshape(ny, pairs, lanes)

    barrier = pltpu.get_barrier_semaphore()
    pl.semaphore_signal(barrier, inc=1, device_id=(partner,), device_id_type=MESH)

    @pl.loop(1, chips)
    def _(k):
        other = flip(chip, k, chips) * 2 + core
        pl.semaphore_signal(barrier, inc=1, device_id=(other,), device_id_type=MESH)

    for p in range(pairs):
        send[pl.ds(p, ny, stride=pairs), :] = points_ref[p].T

    pl.semaphore_wait(barrier, chips)

    def out_copy(k):
        target = flip(chip, k, chips)
        return pltpu.make_async_remote_copy(
            src_ref=rows_of_y.at[pl.ds(wide_base(target), wide)],
            dst_ref=direct.at[k],
            send_sem=send_sem.at[k],
            recv_sem=recv_sem.at[k],
            device_id=(target * 2 + core,),
            device_id_type=MESH,
        )

    def pass_copy(k):
        skip = narrow_base(partner) - wide_base(chip)
        return pltpu.make_async_remote_copy(
            src_ref=direct.at[k, pl.ds(skip, narrow)],
            dst_ref=passed.at[k],
            send_sem=pass_send_sem.at[k],
            recv_sem=pass_recv_sem.at[k],
            device_id=(partner,),
            device_id_type=MESH,
        )

    @pl.loop(1, chips)
    def _(k):
        out_copy(k).start()

    own = pl.ds(wide_base(chip), wide)
    stay = pltpu.make_async_copy(rows_of_y.at[own], direct.at[0], recv_sem.at[0])
    stay.start()

    make_weights(dims, me, span_base, oy_ref, cy_ref, oz_ref, cz_ref, cx_ref, wx_ref, wy, rz, rz_lo)

    def from_direct(place, k):
        refine_y(
            jl, pairs, span_base, wy, mixed, place,
            lambda row: direct[k, row],
            wide_base(chip),
        )
        return flip(chip, k, chips) * 2 + core

    def from_passed(place, k):
        refine_y(
            jl, pairs, span_base, wy, mixed, place,
            lambda row: passed[k, row],
            narrow_base(me),
        )
        return flip(chip, k, chips) * 2 + 1 - core

    stay.wait()
    pass_copy(0).start()
    refine_z(dims, pairs, mixed, rz, rz_lo, grid_ref, [from_direct(0, 0)])

    @pl.loop(1, chips)
    def _(k):
        out_copy(k).wait_recv()
        pass_copy(k).start()
        one = from_direct(0, k)
        pass_copy(k - 1).wait_recv()
        two = from_passed(1, k - 1)
        refine_z(dims, pairs, mixed, rz, rz_lo, grid_ref, [one, two])

    pass_copy(chips - 1).wait_recv()
    refine_z(dims, pairs, mixed, rz, rz_lo, grid_ref, [from_passed(0, chips - 1)])

    @pl.loop(1, chips)
    def _(k):
        out_copy(k).wait_send()

    @pl.loop(0, chips)
    def _(k):
        pass_copy(k).wait_send()


def relay(
    dims,
    points_hbm, oy_hbm, cy_hbm, oz_hbm, cz_hbm, cx_hbm, ox_hbm,
    block_ref,
    slab, send, direct, passed, wy, rz, rz_lo, mixed,
    oy_ref, cy_ref, oz_ref, cz_ref, cx_ref,
    grid_ref, ox_ref, wx_ref, wx_scalars,
    load_sem, small_sem, out_sem, hand_sem, pass_sem,
    whole_recv, low_recv, high_recv, middle_recv, pass_recv,
    flags, partner_flag,
):
    n, comps, xl, ny, nz, jl, mz = dims
    chips = n // 2
    plane = chips // PLANES
    pairs, lanes = slab.shape[0], slab.shape[1]
    own, half = jl, jl // 2
    wide, narrow = own + REACH, half + REACH
    whole, low, high = pl.ds(0, wide), pl.ds(0, REACH), pl.ds(own, REACH)
    middle = pl.ds(REACH, own - REACH)
    low_inside, high_inside = pl.ds(BELOW, ABOVE), pl.ds(own, BELOW)
    me = lax.axis_index("slab")
    chip, core = lax.div(me, 2), lax.rem(me, 2)
    partner = chip * 2 + 1 - core
    here, level = lax.rem(chip, plane), lax.div(chip, plane)
    rows_of_y = send.reshape(ny + REACH, pairs, lanes)
    any_rows = direct.reshape(PLANES * plane * wide, pairs, lanes)
    span_base = functools.partial(span_of, me, jl, ny)
    around = [flip(here, d, plane) for d in range(plane)]

    loads = [pltpu.make_async_copy(points_hbm.at[p], slab.at[p], load_sem.at[p]) for p in range(pairs)]
    for load in loads:
        load.start()

    barrier = pltpu.get_barrier_semaphore()

    def greet(semaphore, device):
        pl.semaphore_signal(semaphore, inc=1, device_id=(device,), device_id_type=MESH)

    def device_of(z, q):
        return (z * plane + q) * 2 + core

    side = [lax.rem(here, 2), lax.div(here, 2)]
    above = [None, side[0] == 0, side[1] == 0, side[0] + side[1] == 0]
    below = [None, side[0] == 1, side[1] == 1, side[0] + side[1] == 2]
    missing = [None, side[0] == 0, side[1] == 0, side[0] + side[1] < 2]

    @pl.when(core == 0)
    def _():
        greet(barrier, partner)

    for d in range(plane):
        def hail(d=d):
            @pl.loop(level + (d == 0), PLANES)
            def _(z):
                greet(barrier, device_of(z, around[d]))

        hail() if d == 0 else pl.when(above[d])(hail)

    smalls = [
        pltpu.make_async_copy(src, dst, small_sem.at[i])
        for i, (src, dst) in enumerate(
            [(oy_hbm, oy_ref), (cy_hbm, cy_ref), (oz_hbm, oz_ref), (cz_hbm, cz_ref), (cx_hbm, cx_ref), (ox_hbm, ox_ref)]
        )
    ]
    for small in smalls:
        small.start()

    @pl.when(me > 0)
    def _():
        pl.semaphore_wait(barrier, (level + 1) * (1 + side[0]) * (1 + side[1]) - 1 + core)

    for d in range(plane):
        def answer(d=d):
            @pl.loop(0, level + (d != 0))
            def _(z):
                greet(flags.at[chip], device_of(z, around[d]))

        answer() if d == 0 else pl.when(below[d])(answer)

    def introduce(za, qa, zb, qb):
        greet(flags.at[zb * plane + qb], device_of(za, qa))
        greet(flags.at[za * plane + qa], device_of(zb, qb))

    for q in range(1, plane):
        @pl.when(here == q)
        def _():
            if q == plane - 1:
                introduce(level, 1, level, 2)

            @pl.loop(0, level)
            def _(z):
                for low_q in range(plane):
                    for high_q in range(plane):
                        if low_q | high_q == q and high_q != q:
                            if low_q & ~high_q:
                                introduce(z, low_q, level, high_q)

    @pl.when(core == 1)
    def _():
        greet(partner_flag, partner)

    for edge in (pl.ds(0, BELOW), pl.ds(BELOW + ny, ABOVE)):
        rows_of_y[edge] = jnp.zeros((edge.size, pairs, lanes), jnp.float32)
    for load in loads:
        load.wait()
    for p in range(pairs):
        send[pl.ds(BELOW * pairs + p, ny, stride=pairs), :] = slab[p].T

    def remote(src, dst, send_sem, recv_sem, device):
        return pltpu.make_async_remote_copy(
            src_ref=src, dst_ref=dst, send_sem=send_sem, recv_sem=recv_sem,
            device_id=(device,), device_id_type=MESH,
        )

    def await_recv(ref, semaphore):
        remote(ref, ref, out_sem, semaphore, partner).wait_recv()

    def await_send(count, semaphore):
        rows = any_rows.at[pl.ds(0, count)]
        remote(rows, rows, semaphore, pass_recv.at[0], partner).wait_send()

    def put(z, q, rows, semaphores):
        remote(
            rows_of_y.at[pl.ds((z * plane + q) * own + rows.start, rows.size)],
            direct.at[level, here, rows], out_sem, semaphores.at[level],
            (z * plane + q) * 2 + core,
        ).start()

    lacking = [None, side[0] == 0, side[1] == 0, here < plane - 1]

    def pick(mine, z, i):
        if z < mine:
            q, unknown = i, lacking[i]
        else:
            q, unknown = around[i], True if z > mine else missing[i]

        def wait():
            pl.semaphore_wait(flags.at[z * plane + q], 1)

        if unknown is True:
            wait()
        elif unknown is not None:
            pl.when(unknown)(wait)
        return q

    def send_whole(mine, z, places):
        for i in places:
            put(z, pick(mine, z, i), whole, whole_recv)

    def send_ends(mine, z, places):
        for i in places:
            q = pick(mine, z, i)
            if z == 0:
                pl.when(q == 0)(functools.partial(put, z, q, low_inside, low_recv))
                pl.when(q > 0)(functools.partial(put, z, q, low, low_recv))
            else:
                put(z, q, low, low_recv)
            edge = high_inside if z == PLANES - 1 else high
            pl.when(q == plane - 1)(functools.partial(put, z, q, edge, high_recv))

    def send_middle(mine, z, places):
        for i in places if z < mine else places[::-1]:
            put(z, i if z < mine else around[i], middle, middle_recv)

    def pass_copy(z):
        return remote(
            direct.at[z, :, pl.ds((1 - core) * half, narrow)], passed.at[z],
            pass_sem, pass_recv.at[z], partner,
        )

    def refine(blocks, base, devices):
        for j in range(jl):
            row = span_base(j) - base
            sums = [None] * len(blocks)
            for m in range(SPAN):
                weight = wy[j * SPAN + m]
                for i, block in enumerate(blocks):
                    term = weight * block[row + m]
                    sums[i] = term if m == 0 else sums[i] + term
            for i, total in enumerate(sums):
                mixed[pl.ds(i * pairs * jl + j, pairs, stride=jl), :] = total
        refine_z(dims, pairs, mixed, rz, rz_lo, grid_ref, devices)

    def take_whole(z):
        await_recv(direct.at[z], whole_recv.at[z])
        pass_copy(z).start()

    def take_plane(z):
        await_recv(direct.at[z, pl.ds(0, plane - 1)], whole_recv.at[z])
        pass_copy(z).start()

    def take_low(z):
        @pl.when(chip > 0)
        def _():
            await_recv(direct.at[z, :, low], low_recv.at[z])

        @pl.when(chip == 0)
        def _():
            await_recv(direct.at[z, :, low_inside], low_recv.at[z])

        @pl.when(here > 0)
        def _():
            remote(
                direct.at[z, :, low], direct.at[z, :, high], hand_sem, high_recv.at[z], (chip - 1) * 2 + core
            ).start()

    def take_middle(z):
        @pl.when(chip < chips - 1)
        def _():
            await_recv(direct.at[z, :, high], high_recv.at[z])

        @pl.when(chip == chips - 1)
        def _():
            await_recv(direct.at[z, :, high_inside], high_recv.at[z])

        await_recv(direct.at[z, :, middle], middle_recv.at[z])
        pass_copy(z).start()

    def near(z):
        refine(
            [direct.at[z, q] for q in range(plane)], chip * own - BELOW,
            [(z * plane + q) * 2 + core for q in range(plane)],
        )

    def far(z):
        pass_copy(z).wait_recv()
        refine(
            [passed.at[z, q] for q in range(plane)], me * half - BELOW,
            [(z * plane + q) * 2 + 1 - core for q in range(plane)],
        )

    mx, nx = wx_ref.shape[1], n * xl
    depth = nx // PLANES

    def across(known, written):
        fresh = []
        for g in range(mx // GROUP):
            low_x = max(g * GROUP // 2 - BELOW, 0)
            high_x = min((g * GROUP + GROUP - 1) // 2 + ABOVE, nx - 1)
            if g not in written and set(range(low_x // depth, high_x // depth + 1)) <= known:
                fresh.append(g)
        written.update(fresh)
        starts = [g for g in fresh if g - 1 not in fresh]
        for start in starts:
            stop = start
            while stop in fresh:
                stop += 1
            refine_rows(start, stop)

    def refine_rows(start, stop):
        @pl.loop(start, stop)
        def _(g):
            done = []
            for r in range(GROUP):
                i = g * GROUP + r
                first = ox_ref[i]
                weights = [wx_scalars[k, i] for k in range(BAND)]
                for c in range(comps):
                    acc = weights[0] * grid_ref[c, first]
                    for k in range(1, BAND):
                        acc = acc + weights[k] * grid_ref[c, first + k]
                    done.append((c, i, acc))
            for c, i, acc in done:
                block_ref[c, i] = acc

    acts = {
        "W": send_whole, "E": send_ends, "M": send_middle,
        "w": take_whole, "p": take_plane, "e": take_low, "m": take_middle, "n": near, "f": far,
    }
    sends = [
        ["W0:123", "W1", "E2", "E3", "M3", "M2"],
        ["W0", "W1:123", "E2", "E3", "M3", "M2"],
        ["E0:012", "E1:012", "E0:3", "E1:3", "W2:123", "W3", "M0", "M1"],
        ["E0:012", "E1:012", "E0:3", "E1:3", "W2", "W3:123", "M0", "M1"],
    ]
    takes = [
        ["p0", "n0", "e2", "f0", "w1", "n1", "e3", "f1", "x", "m2", "n2", "m3", "f2", "x", "n3", "f3", "x"],
        ["p1", "n1", "w0", "n0", "f1", "e3", "f0", "x", "e2", "m3", "n3", "m2", "f3", "n2", "x", "f2", "x"],
        ["p2", "n2", "e1", "f2", "e0", "w3", "n3", "f3", "x", "m0", "n0", "m1", "f0", "n1", "x", "f1", "x"],
        ["p3", "n3", "w2", "n2", "f3", "e0", "f2", "x", "e1", "m0", "n0", "m1", "f0", "n1", "x", "f1", "x"],
    ]

    for z, plan in enumerate(sends):

        @pl.when(level == z)
        def _():
            for step in plan:
                target, _, places = step[1:].partition(":")
                acts[step[0]](z, int(target), [int(i) for i in places] or list(range(plane)))

    direct[level, here] = rows_of_y[pl.ds(chip * own, wide)]

    @pl.when(core == 0)
    def _():
        pl.semaphore_wait(partner_flag, 1)

    for small in smalls:
        small.wait()
    make_weights(dims, me, span_base, oy_ref, cy_ref, oz_ref, cz_ref, cx_ref, wx_ref, wy, rz, rz_lo)
    scalars = pltpu.make_async_copy(wx_ref, wx_scalars, small_sem.at[0])
    scalars.start()
    scalars.wait()

    for z, plan in enumerate(takes):

        @pl.when(level == z)
        def _():
            known, written = set(), set()
            for step in plan:
                if step == "x":
                    across(known, written)
                else:
                    acts[step[0]](int(step[1]))
                    known |= {int(step[1])} if step[0] == "f" else set()
            assert len(written) == mx // GROUP

    ends = 2 * (plane * own + REACH) + (2 * plane - 1) * wide

    @pl.when(lax.div(level, 2) == 0)
    def _():
        await_send(ends - ABOVE, out_sem)

    @pl.when(lax.div(level, 2) == 1)
    def _():
        await_send(ends - BELOW, out_sem)

    @pl.when(here > 0)
    def _():
        await_send(2 * plane * REACH, hand_sem)

    await_send(PLANES * plane * narrow, pass_sem)


def refine_x(steps, ox_ref, wx_ref, grid_ref, out_ref, block, sems):
    comps, mx = block.shape[0], block.shape[1]
    rows = mx // steps

    def put(s):
        part = pl.ds(pl.multiple_of(s * rows, rows), rows)
        return pltpu.make_async_copy(block.at[:, part], out_ref.at[:, part], sems.at[s])

    @pl.loop(0, steps)
    def _(s):
        @pl.loop(0, rows // GROUP)
        def _(g):
            done = []
            for q in range(GROUP):
                i = s * rows + g * GROUP + q
                first = ox_ref[i]
                weights = [wx_ref[k, i] for k in range(BAND)]
                for c in range(comps):
                    acc = weights[0] * grid_ref[c, first]
                    for k in range(1, BAND):
                        acc = acc + weights[k] * grid_ref[c, first + k]
                    done.append((c, i, acc))
            for c, i, acc in done:
                block[c, i] = acc

        put(s).start()

    @pl.loop(0, steps)
    def _(s):
        put(s).wait()


def store(block_ref, out_ref, sems):
    copies = [pltpu.make_async_copy(block_ref.at[c], out_ref.at[c], sems.at[c]) for c in range(block_ref.shape[0])]
    for copy in copies:
        copy.start()
    for copy in copies:
        copy.wait()


def solution(mesh):
    n = mesh.shape["slab"]
    vmem = pl.BlockSpec(memory_space=pltpu.VMEM)
    smem = pl.BlockSpec(memory_space=pltpu.SMEM)

    def body(points, offsets_x, coeffs_x, offsets_y, coeffs_y, offsets_z, coeffs_z):
        comps, xl, ny, nz = points.shape
        nx = xl * n
        mx, my, mz = offsets_x.shape[0], offsets_y.shape[0], offsets_z.shape[0]
        jl = my // n
        fold = 128 // nz
        pairs = comps * xl // fold
        lanes = fold * nz
        chips = n // 2
        cl = jl // 2
        wide, narrow = 2 * cl + REACH, cl + REACH
        slab = jnp.transpose(points, (0, 1, 3, 2)).reshape(pairs, lanes, ny)
        f32, bf16 = jnp.float32, jnp.bfloat16
        f32_rows = lambda *shape: pltpu.VMEM((*shape, pairs, lanes), f32)
        shared = [
            pltpu.VMEM((jl * SPAN, pairs, lanes), f32),
            pltpu.VMEM((2 * lanes, fold * mz), bf16),
            pltpu.VMEM((lanes, fold * mz), bf16),
            pltpu.VMEM((4 * pairs * jl, lanes), f32),
        ]
        semaphores = lambda *shape: pltpu.SemaphoreType.DMA(shape)
        if jl > REACH and chips == PLANES * PLANES and my == 2 * ny and mx % (PLANES * GROUP) == 0:
            plane = chips // PLANES
            limit = VMEM_MOST - 4 * comps * mx * jl * mz
            hbm = pl.BlockSpec(memory_space=pltpu.HBM)
            block = pl.pallas_call(
                functools.partial(relay, (n, comps, xl, ny, nz, jl, mz)),
                out_shape=pltpu.VMEM((comps, mx, jl, mz), f32),
                in_specs=[hbm] * 7,
                out_specs=vmem,
                scratch_shapes=[
                    pltpu.VMEM((pairs, lanes, ny), f32),
                    pltpu.VMEM(((ny + REACH) * pairs, lanes), f32),
                    f32_rows(PLANES, plane, jl + REACH),
                    f32_rows(PLANES, plane, cl + REACH),
                    *shared,
                    pltpu.SMEM((my,), jnp.int32),
                    pltpu.SMEM((BAND, my), f32),
                    pltpu.VMEM((1, mz), jnp.int32),
                    pltpu.VMEM((BAND, mz), f32),
                    pltpu.VMEM((BAND, mx), f32),
                    pltpu.VMEM((comps, nx, jl, mz), f32),
                    pltpu.SMEM((mx,), jnp.int32),
                    pltpu.VMEM((BAND, mx), f32),
                    pltpu.SMEM((BAND, mx), f32),
                    semaphores(pairs),
                    semaphores(6),
                    *[pltpu.SemaphoreType.DMA] * 3,
                    *[semaphores(PLANES)] * 5,
                    pltpu.SemaphoreType.REGULAR((chips,)),
                    pltpu.SemaphoreType.REGULAR,
                ],
                compiler_params=pltpu.CompilerParams(
                    collective_id=0, has_side_effects=True, vmem_limit_bytes=limit
                ),
                name="relay",
            )(slab, offsets_y, coeffs_y, offsets_z.reshape(1, mz), coeffs_z, coeffs_x, offsets_x)
            return pl.pallas_call(
                store,
                out_shape=jax.ShapeDtypeStruct((comps, mx, jl, mz), f32),
                in_specs=[vmem],
                out_specs=pl.BlockSpec(memory_space=pltpu.HBM),
                scratch_shapes=[semaphores(comps)],
                compiler_params=pltpu.CompilerParams(vmem_limit_bytes=limit),
                name="store",
            )(pltpu.with_memory_space_constraint(block, pltpu.VMEM))
        grid, wx = pl.pallas_call(
            functools.partial(exchange, (n, comps, xl, ny, nz, jl, mz)),
            out_shape=(
                pltpu.VMEM((comps, nx, jl, mz), f32),
                jax.ShapeDtypeStruct((BAND, mx), f32),
            ),
            in_specs=[vmem, smem, smem, vmem, vmem, vmem],
            out_specs=(vmem, vmem),
            scratch_shapes=[
                pltpu.VMEM((ny * pairs, lanes), f32),
                f32_rows(chips, wide),
                f32_rows(chips, narrow),
                *shared,
                *[semaphores(chips)] * 4,
            ],
            compiler_params=pltpu.CompilerParams(collective_id=0, has_side_effects=True),
            name="exchange",
        )(slab, offsets_y, coeffs_y, offsets_z.reshape(1, mz), coeffs_z, coeffs_x)
        steps = 8
        return pl.pallas_call(
            functools.partial(refine_x, steps),
            out_shape=jax.ShapeDtypeStruct((comps, mx, jl, mz), f32),
            in_specs=[smem, smem, vmem],
            out_specs=pl.BlockSpec(memory_space=pltpu.HBM),
            scratch_shapes=[
                pltpu.VMEM((comps, mx, jl, mz), f32),
                pltpu.SemaphoreType.DMA((steps,)),
            ],
            name="refine_x",
        )(offsets_x, wx, pltpu.with_memory_space_constraint(grid, pltpu.VMEM))

    return jax.shard_map(
        body,
        mesh=mesh,
        in_specs=(P(None, "slab", None, None), P(), P(), P(), P(), P(), P()),
        out_specs=P(None, None, "slab", None),
        check_vma=False,
    )
```

```python
import functools

import jax
import jax.numpy as jnp
from jax import lax
from jax.experimental import pallas as pl
from jax.experimental.pallas import tpu as pltpu
from jax.sharding import PartitionSpec as P

MESH = pl.DeviceIdType.MESH
BAND = 4
REACH = BAND + 1
SPAN = BAND + 2
BELOW, ABOVE = 2, 3
PLANES = 4
GROUP = 8
VMEM_MOST = 67043328
LAST = (3, 2, 1, 1)


def flip(a, k, chips):
    out = 0
    bit = 1
    while bit < chips:
        a_bit, k_bit = lax.rem(lax.div(a, bit), 2), (k // bit) % 2
        out = out + (a_bit + k_bit - 2 * a_bit * k_bit) * bit
        bit *= 2
    return out


def span_of(me, jl, ny, j):
    return jnp.clip((me * jl + j) // 2 - 2, 0, ny - SPAN)


def make_weights(dims, me, span_base, oy_ref, cy_ref, oz_ref, cz_ref, cx_ref, wx_ref, wy, rz, rz_lo):
    n, comps, xl, ny, nz, jl, mz = dims
    pairs, lanes = wy.shape[1], wy.shape[2]
    fold = lanes // nz
    wx_ref[...] = cx_ref[...] / jnp.sum(cx_ref[...], axis=0, keepdims=True)
    wz = cz_ref[...] / jnp.sum(cz_ref[...], axis=0, keepdims=True)
    at = lax.broadcasted_iota(jnp.int32, (nz, mz), 0)
    first = jnp.broadcast_to(oz_ref[...], (nz, mz))
    band = jnp.zeros((nz, mz), jnp.float32)
    for k in range(BAND):
        band = band + jnp.where(at == first + k, jnp.broadcast_to(wz[k : k + 1], (nz, mz)), 0.0)
    high = band.astype(jnp.bfloat16)
    low = (band - high.astype(jnp.float32)).astype(jnp.bfloat16)
    rz[...] = jnp.zeros_like(rz)
    rz_lo[...] = jnp.zeros_like(rz_lo)
    for f in range(fold):
        rz[f * nz : (f + 1) * nz, f * mz : (f + 1) * mz] = high
        rz[lanes + f * nz : lanes + (f + 1) * nz, f * mz : (f + 1) * mz] = high
        rz_lo[f * nz : (f + 1) * nz, f * mz : (f + 1) * mz] = low
    for j in range(jl):
        coeffs = [jnp.full((pairs, lanes), cy_ref[k, me * jl + j]) for k in range(BAND)]
        total = coeffs[0] + coeffs[1] + coeffs[2] + coeffs[3]
        coeffs = [c / total for c in coeffs]
        skip = jnp.full((pairs, lanes), oy_ref[me * jl + j] - span_base(j))
        for m in range(SPAN):
            weight = jnp.zeros((pairs, lanes), jnp.float32)
            for k in range(max(0, m - SPAN + BAND), min(BAND, m + 1)):
                weight = jnp.where(skip == m - k, coeffs[k], weight)
            wy[j * SPAN + m] = weight


def refine_y(jl, pairs, span_base, wy, mixed, place, load, base):
    for j in range(jl):
        row = span_base(j) - base
        acc = wy[j * SPAN] * load(row)
        for m in range(1, SPAN):
            acc = acc + wy[j * SPAN + m] * load(row + m)
        mixed[pl.ds(place * pairs * jl + j, pairs, stride=jl), :] = acc


def refine_z(dims, pairs, mixed, rz, rz_lo, grid_ref, devices):
    n, comps, xl, ny, nz, jl, mz = dims
    fold = mixed.shape[1] // nz
    rows = pairs * jl * len(devices)
    x = mixed[:rows]
    hi = x.astype(jnp.bfloat16)
    lo = (x - hi.astype(jnp.float32)).astype(jnp.bfloat16)
    both = jnp.concatenate([hi, lo], axis=1)
    res = jnp.dot(both, rz[...], preferred_element_type=jnp.float32)
    res = res + jnp.dot(hi, rz_lo[...], preferred_element_type=jnp.float32)
    per = pairs // comps
    for q, device in enumerate(devices):
        for p in range(pairs):
            for f in range(fold):
                spot = (p // per, device * xl + (p % per) * fold + f)
                top = (q * pairs + p) * jl
                grid_ref[spot] = res[top : top + jl, f * mz : (f + 1) * mz]


def exchange(
    dims,
    points_ref, oy_ref, cy_ref, oz_ref, cz_ref, cx_ref,
    grid_ref, wx_ref,
    send, direct, passed, wy, rz, rz_lo, mixed,
    send_sem, recv_sem, pass_send_sem, pass_recv_sem,
):
    n, comps, xl, ny, nz, jl, mz = dims
    chips = n // 2
    pairs, lanes = points_ref.shape[0], points_ref.shape[1]
    cl = jl // 2
    wide, narrow = 2 * cl + REACH, cl + REACH
    me = lax.axis_index("slab")
    chip, core = me // 2, me % 2
    partner = chip * 2 + 1 - core

    def wide_base(c):
        return jnp.clip(c * 2 * cl - 2, 0, ny - wide)

    def narrow_base(d):
        return jnp.clip(d * cl - 2, 0, ny - narrow)

    span_base = functools.partial(span_of, me, jl, ny)

    rows_of_y = send.reshape(ny, pairs, lanes)

    barrier = pltpu.get_barrier_semaphore()
    pl.semaphore_signal(barrier, inc=1, device_id=(partner,), device_id_type=MESH)

    @pl.loop(1, chips)
    def _(k):
        other = flip(chip, k, chips) * 2 + core
        pl.semaphore_signal(barrier, inc=1, device_id=(other,), device_id_type=MESH)

    for p in range(pairs):
        send[pl.ds(p, ny, stride=pairs), :] = points_ref[p].T

    pl.semaphore_wait(barrier, chips)

    def out_copy(k):
        target = flip(chip, k, chips)
        return pltpu.make_async_remote_copy(
            src_ref=rows_of_y.at[pl.ds(wide_base(target), wide)],
            dst_ref=direct.at[k],
            send_sem=send_sem.at[k],
            recv_sem=recv_sem.at[k],
            device_id=(target * 2 + core,),
            device_id_type=MESH,
        )

    def pass_copy(k):
        skip = narrow_base(partner) - wide_base(chip)
        return pltpu.make_async_remote_copy(
            src_ref=direct.at[k, pl.ds(skip, narrow)],
            dst_ref=passed.at[k],
            send_sem=pass_send_sem.at[k],
            recv_sem=pass_recv_sem.at[k],
            device_id=(partner,),
            device_id_type=MESH,
        )

    @pl.loop(1, chips)
    def _(k):
        out_copy(k).start()

    own = pl.ds(wide_base(chip), wide)
    stay = pltpu.make_async_copy(rows_of_y.at[own], direct.at[0], recv_sem.at[0])
    stay.start()

    make_weights(dims, me, span_base, oy_ref, cy_ref, oz_ref, cz_ref, cx_ref, wx_ref, wy, rz, rz_lo)

    def from_direct(place, k):
        refine_y(
            jl, pairs, span_base, wy, mixed, place,
            lambda row: direct[k, row],
            wide_base(chip),
        )
        return flip(chip, k, chips) * 2 + core

    def from_passed(place, k):
        refine_y(
            jl, pairs, span_base, wy, mixed, place,
            lambda row: passed[k, row],
            narrow_base(me),
        )
        return flip(chip, k, chips) * 2 + 1 - core

    stay.wait()
    pass_copy(0).start()
    refine_z(dims, pairs, mixed, rz, rz_lo, grid_ref, [from_direct(0, 0)])

    @pl.loop(1, chips)
    def _(k):
        out_copy(k).wait_recv()
        pass_copy(k).start()
        one = from_direct(0, k)
        pass_copy(k - 1).wait_recv()
        two = from_passed(1, k - 1)
        refine_z(dims, pairs, mixed, rz, rz_lo, grid_ref, [one, two])

    pass_copy(chips - 1).wait_recv()
    refine_z(dims, pairs, mixed, rz, rz_lo, grid_ref, [from_passed(0, chips - 1)])

    @pl.loop(1, chips)
    def _(k):
        out_copy(k).wait_send()

    @pl.loop(0, chips)
    def _(k):
        pass_copy(k).wait_send()


def relay(
    dims,
    points_hbm, oy_hbm, cy_hbm, oz_hbm, cz_hbm, cx_hbm, ox_hbm,
    block_ref, grid_ref, wx_ref,
    slab, send, direct, passed, wy, rz, rz_lo, mixed,
    oy_ref, cy_ref, oz_ref, cz_ref, cx_ref,
    ox_ref, wx_scalars,
    load_sem, small_sem, out_sem, hand_sem, pass_sem,
    whole_recv, low_recv, high_recv, middle_recv, pass_recv,
    flags, partner_flag,
):
    n, comps, xl, ny, nz, jl, mz = dims
    chips = n // 2
    plane = chips // PLANES
    pairs, lanes = slab.shape[0], slab.shape[1]
    own, half = jl, jl // 2
    wide, narrow = own + REACH, half + REACH
    whole, low, high = pl.ds(0, wide), pl.ds(0, REACH), pl.ds(own, REACH)
    middle = pl.ds(REACH, own - REACH)
    low_inside, high_inside = pl.ds(BELOW, ABOVE), pl.ds(own, BELOW)
    me = lax.axis_index("slab")
    chip, core = lax.div(me, 2), lax.rem(me, 2)
    partner = chip * 2 + 1 - core
    here, level = lax.rem(chip, plane), lax.div(chip, plane)
    rows_of_y = send.reshape(ny + REACH, pairs, lanes)
    any_rows = direct.reshape(PLANES * plane * wide, pairs, lanes)
    span_base = functools.partial(span_of, me, jl, ny)
    around = [flip(here, d, plane) for d in range(plane)]

    loads = [pltpu.make_async_copy(points_hbm.at[p], slab.at[p], load_sem.at[p]) for p in range(pairs)]
    for load in loads:
        load.start()

    barrier = pltpu.get_barrier_semaphore()

    def greet(semaphore, device):
        pl.semaphore_signal(semaphore, inc=1, device_id=(device,), device_id_type=MESH)

    def device_of(z, q):
        return (z * plane + q) * 2 + core

    side = [lax.rem(here, 2), lax.div(here, 2)]
    above = [None, side[0] == 0, side[1] == 0, side[0] + side[1] == 0]
    below = [None, side[0] == 1, side[1] == 1, side[0] + side[1] == 2]
    missing = [None, side[0] == 0, side[1] == 0, side[0] + side[1] < 2]

    @pl.when(core == 0)
    def _():
        greet(barrier, partner)

    for d in range(plane):
        def hail(d=d):
            @pl.loop(level + (d == 0), PLANES)
            def _(z):
                greet(barrier, device_of(z, around[d]))

        hail() if d == 0 else pl.when(above[d])(hail)

    smalls = [
        pltpu.make_async_copy(src, dst, small_sem.at[i])
        for i, (src, dst) in enumerate(
            [(oy_hbm, oy_ref), (cy_hbm, cy_ref), (oz_hbm, oz_ref), (cz_hbm, cz_ref), (cx_hbm, cx_ref), (ox_hbm, ox_ref)]
        )
    ]
    for small in smalls:
        small.start()

    @pl.when(me > 0)
    def _():
        pl.semaphore_wait(barrier, (level + 1) * (1 + side[0]) * (1 + side[1]) - 1 + core)

    for d in range(plane):
        def answer(d=d):
            @pl.loop(0, level + (d != 0))
            def _(z):
                greet(flags.at[chip], device_of(z, around[d]))

        answer() if d == 0 else pl.when(below[d])(answer)

    def introduce(za, qa, zb, qb):
        greet(flags.at[zb * plane + qb], device_of(za, qa))
        greet(flags.at[za * plane + qa], device_of(zb, qb))

    for q in range(1, plane):
        @pl.when(here == q)
        def _():
            if q == plane - 1:
                introduce(level, 1, level, 2)

            @pl.loop(0, level)
            def _(z):
                for low_q in range(plane):
                    for high_q in range(plane):
                        if low_q | high_q == q and high_q != q:
                            if low_q & ~high_q:
                                introduce(z, low_q, level, high_q)

    @pl.when(core == 1)
    def _():
        greet(partner_flag, partner)

    for edge in (pl.ds(0, BELOW), pl.ds(BELOW + ny, ABOVE)):
        rows_of_y[edge] = jnp.zeros((edge.size, pairs, lanes), jnp.float32)
    for load in loads:
        load.wait()
    for p in range(pairs):
        send[pl.ds(BELOW * pairs + p, ny, stride=pairs), :] = slab[p].T

    def remote(src, dst, send_sem, recv_sem, device):
        return pltpu.make_async_remote_copy(
            src_ref=src, dst_ref=dst, send_sem=send_sem, recv_sem=recv_sem,
            device_id=(device,), device_id_type=MESH,
        )

    def await_recv(ref, semaphore):
        remote(ref, ref, out_sem, semaphore, partner).wait_recv()

    def await_send(count, semaphore):
        rows = any_rows.at[pl.ds(0, count)]
        remote(rows, rows, semaphore, pass_recv.at[0], partner).wait_send()

    def put(z, q, rows, semaphores):
        remote(
            rows_of_y.at[pl.ds((z * plane + q) * own + rows.start, rows.size)],
            direct.at[level, here, rows], out_sem, semaphores.at[level],
            (z * plane + q) * 2 + core,
        ).start()

    lacking = [None, side[0] == 0, side[1] == 0, here < plane - 1]

    def pick(mine, z, i):
        if z < mine:
            q, unknown = i, lacking[i]
        else:
            q, unknown = around[i], True if z > mine else missing[i]

        def wait():
            pl.semaphore_wait(flags.at[z * plane + q], 1)

        if unknown is True:
            wait()
        elif unknown is not None:
            pl.when(unknown)(wait)
        return q

    def send_whole(mine, z, places):
        for i in places:
            put(z, pick(mine, z, i), whole, whole_recv)

    def send_ends(mine, z, places):
        for i in places:
            q = pick(mine, z, i)
            if z == 0:
                pl.when(q == 0)(functools.partial(put, z, q, low_inside, low_recv))
                pl.when(q > 0)(functools.partial(put, z, q, low, low_recv))
            else:
                put(z, q, low, low_recv)
            edge = high_inside if z == PLANES - 1 else high
            pl.when(q == plane - 1)(functools.partial(put, z, q, edge, high_recv))

    def send_middle(mine, z, places):
        for i in places if z < mine else places[::-1]:
            put(z, i if z < mine else around[i], middle, middle_recv)

    def pass_copy(z):
        return remote(
            direct.at[z, :, pl.ds((1 - core) * half, narrow)], passed.at[z],
            pass_sem, pass_recv.at[z], partner,
        )

    def refine(blocks, base, devices):
        for j in range(jl):
            row = span_base(j) - base
            sums = [None] * len(blocks)
            for m in range(SPAN):
                weight = wy[j * SPAN + m]
                for i, block in enumerate(blocks):
                    term = weight * block[row + m]
                    sums[i] = term if m == 0 else sums[i] + term
            for i, total in enumerate(sums):
                mixed[pl.ds(i * pairs * jl + j, pairs, stride=jl), :] = total
        refine_z(dims, pairs, mixed, rz, rz_lo, grid_ref, devices)

    def take_whole(z):
        await_recv(direct.at[z], whole_recv.at[z])
        pass_copy(z).start()

    def take_plane(z):
        await_recv(direct.at[z, pl.ds(0, plane - 1)], whole_recv.at[z])
        pass_copy(z).start()

    def take_low(z):
        @pl.when(chip > 0)
        def _():
            await_recv(direct.at[z, :, low], low_recv.at[z])

        @pl.when(chip == 0)
        def _():
            await_recv(direct.at[z, :, low_inside], low_recv.at[z])

        @pl.when(here > 0)
        def _():
            remote(
                direct.at[z, :, low], direct.at[z, :, high], hand_sem, high_recv.at[z], (chip - 1) * 2 + core
            ).start()

    def take_middle(z):
        @pl.when(chip < chips - 1)
        def _():
            await_recv(direct.at[z, :, high], high_recv.at[z])

        @pl.when(chip == chips - 1)
        def _():
            await_recv(direct.at[z, :, high_inside], high_recv.at[z])

        await_recv(direct.at[z, :, middle], middle_recv.at[z])
        pass_copy(z).start()

    def near(z):
        refine(
            [direct.at[z, q] for q in range(plane)], chip * own - BELOW,
            [(z * plane + q) * 2 + core for q in range(plane)],
        )

    def far(z):
        pass_copy(z).wait_recv()
        refine(
            [passed.at[z, q] for q in range(plane)], me * half - BELOW,
            [(z * plane + q) * 2 + 1 - core for q in range(plane)],
        )

    mx, nx = wx_ref.shape[1], n * xl

    def across(known, written):
        fresh = groups_in(known, mx, nx) - written
        written |= fresh
        for start, stop in runs(fresh):
            refine_rows(start, stop, ox_ref, wx_scalars, grid_ref, block_ref)

    acts = {
        "W": send_whole, "E": send_ends, "M": send_middle,
        "w": take_whole, "p": take_plane, "e": take_low, "m": take_middle, "n": near, "f": far,
    }
    sends = [
        ["W1:0", "W0:123", "E2", "E3", "W1:123", "M3", "M2"],
        ["W0", "W1:123", "E2", "E3", "M3", "M2"],
        ["W3:0", "E0:012", "E1:012", "W3:12", "E0:3", "E1:3", "W3:3", "W2:123", "M0", "M1"],
        ["E0:012", "E1:012", "E0:3", "E1:3", "W2", "W3:123", "M0", "M1"],
    ]
    takes = [
        ["p0", "n0", "e2", "f0", "w1", "n1", "e3", "f1", "x", "m2", "n2", "m3", "f2", "x", "n3", "f3"],
        ["p1", "n1", "e3", "f1", "w0", "n0", "e2", "f0", "x", "m3", "n3", "m2", "f3", "n2", "x", "f2"],
        ["p2", "n2", "e1", "f2", "e0", "w3", "n3", "f3", "x", "m0", "n0", "m1", "f0", "n1", "x", "f1"],
        ["p3", "n3", "w2", "n2", "f3", "e0", "f2", "x", "e1", "m0", "n0", "m1", "f0", "n1", "x", "f1"],
    ]

    for z, plan in enumerate(sends):

        @pl.when(level == z)
        def _():
            for step in plan:
                target, _, places = step[1:].partition(":")
                acts[step[0]](z, int(target), [int(i) for i in places] or list(range(plane)))

    direct[level, here] = rows_of_y[pl.ds(chip * own, wide)]

    @pl.when(core == 0)
    def _():
        pl.semaphore_wait(partner_flag, 1)

    for small in smalls:
        small.wait()
    make_weights(dims, me, span_base, oy_ref, cy_ref, oz_ref, cz_ref, cx_ref, wx_ref, wy, rz, rz_lo)
    scalars = pltpu.make_async_copy(wx_ref, wx_scalars, small_sem.at[0])
    scalars.start()
    scalars.wait()

    for z, plan in enumerate(takes):

        @pl.when(level == z)
        def _():
            known, written = set(), set()
            for step in plan:
                if step == "x":
                    across(known, written)
                else:
                    acts[step[0]](int(step[1]))
                    known |= {int(step[1])} if step[0] == "f" else set()
            assert written == groups_in(set(range(PLANES)) - {LAST[z]}, mx, nx)

    ends = 2 * (plane * own + REACH) + (2 * plane - 1) * wide

    @pl.when(lax.div(level, 2) == 0)
    def _():
        await_send(ends - ABOVE, out_sem)

    @pl.when(lax.div(level, 2) == 1)
    def _():
        await_send(ends - BELOW, out_sem)

    @pl.when(here > 0)
    def _():
        await_send(2 * plane * REACH, hand_sem)

    await_send(PLANES * plane * narrow, pass_sem)


def refine_x(steps, ox_ref, wx_ref, grid_ref, out_ref, block, sems):
    comps, mx = block.shape[0], block.shape[1]
    rows = mx // steps

    def put(s):
        part = pl.ds(pl.multiple_of(s * rows, rows), rows)
        return pltpu.make_async_copy(block.at[:, part], out_ref.at[:, part], sems.at[s])

    @pl.loop(0, steps)
    def _(s):
        @pl.loop(0, rows // GROUP)
        def _(g):
            done = []
            for q in range(GROUP):
                i = s * rows + g * GROUP + q
                first = ox_ref[i]
                weights = [wx_ref[k, i] for k in range(BAND)]
                for c in range(comps):
                    acc = weights[0] * grid_ref[c, first]
                    for k in range(1, BAND):
                        acc = acc + weights[k] * grid_ref[c, first + k]
                    done.append((c, i, acc))
            for c, i, acc in done:
                block[c, i] = acc

        put(s).start()

    @pl.loop(0, steps)
    def _(s):
        put(s).wait()


def groups_in(known, mx, nx):
    depth = nx // PLANES
    inside = set()
    for g in range(mx // GROUP):
        low = max(g * GROUP // 2 - BELOW, 0) // depth
        high = min((g * GROUP + GROUP - 1) // 2 + ABOVE, nx - 1) // depth
        if set(range(low, high + 1)) <= known:
            inside.add(g)
    return inside


def runs(groups):
    out = []
    for start in sorted(g for g in groups if g - 1 not in groups):
        stop = start
        while stop in groups:
            stop += 1
        out.append((start, stop))
    return out


def refine_rows(start, stop, ox_ref, wx_ref, grid_ref, block_ref):
    comps = block_ref.shape[0]

    @pl.loop(start, stop)
    def _(g):
        done = []
        for r in range(GROUP):
            i = g * GROUP + r
            first = ox_ref[i]
            weights = [wx_ref[k, i] for k in range(BAND)]
            for c in range(comps):
                acc = weights[0] * grid_ref[c, first]
                for k in range(1, BAND):
                    acc = acc + weights[k] * grid_ref[c, first + k]
                done.append((c, i, acc))
        for c, i, acc in done:
            block_ref[c, i] = acc


def finish(ready_ref, grid_ref, wx_hbm, ox_hbm, out_ref, late_ref, ox_ref, wx_ref, out_sem, late_sem, small_sem):
    comps, mx = ready_ref.shape[:2]
    nx = grid_ref.shape[1]
    level = lax.div(lax.axis_index("slab"), 2 * PLANES)
    smalls = [
        pltpu.make_async_copy(src, dst, small_sem.at[i])
        for i, (src, dst) in enumerate([(ox_hbm, ox_ref), (wx_hbm, wx_ref)])
    ]
    for small in smalls:
        small.start()

    def put(src, c, start, stop, sem):
        rows = pl.ds(start * GROUP, (stop - start) * GROUP)
        return pltpu.make_async_copy(src.at[c, rows], out_ref.at[c, rows], sem)

    for z in range(PLANES):

        @pl.when(level == z)
        def _():
            ready = groups_in(set(range(PLANES)) - {LAST[z]}, mx, nx)
            late = runs(set(range(mx // GROUP)) - ready)
            early = [
                put(ready_ref, c, start, stop, out_sem.at[c, i])
                for i, (start, stop) in enumerate(runs(ready))
                for c in range(comps)
            ]
            for copy in early:
                copy.start()
            for small in smalls:
                small.wait()
            rest = []
            for i, (start, stop) in enumerate(late):
                refine_rows(start, stop, ox_ref, wx_ref, grid_ref, late_ref)
                rest += [put(late_ref, c, start, stop, late_sem.at[c, i]) for c in range(comps)]
            for copy in rest:
                copy.start()
            for copy in early + rest:
                copy.wait()


def solution(mesh):
    n = mesh.shape["slab"]
    vmem = pl.BlockSpec(memory_space=pltpu.VMEM)
    smem = pl.BlockSpec(memory_space=pltpu.SMEM)

    def body(points, offsets_x, coeffs_x, offsets_y, coeffs_y, offsets_z, coeffs_z):
        comps, xl, ny, nz = points.shape
        nx = xl * n
        mx, my, mz = offsets_x.shape[0], offsets_y.shape[0], offsets_z.shape[0]
        jl = my // n
        fold = 128 // nz
        pairs = comps * xl // fold
        lanes = fold * nz
        chips = n // 2
        cl = jl // 2
        wide, narrow = 2 * cl + REACH, cl + REACH
        slab = jnp.transpose(points, (0, 1, 3, 2)).reshape(pairs, lanes, ny)
        f32, bf16 = jnp.float32, jnp.bfloat16
        f32_rows = lambda *shape: pltpu.VMEM((*shape, pairs, lanes), f32)
        shared = [
            pltpu.VMEM((jl * SPAN, pairs, lanes), f32),
            pltpu.VMEM((2 * lanes, fold * mz), bf16),
            pltpu.VMEM((lanes, fold * mz), bf16),
            pltpu.VMEM((4 * pairs * jl, lanes), f32),
        ]
        semaphores = lambda *shape: pltpu.SemaphoreType.DMA(shape)
        if jl > REACH and chips == PLANES * PLANES and my == 2 * ny and mx % (PLANES * GROUP) == 0:
            plane = chips // PLANES
            limit = VMEM_MOST - 4 * (comps * (mx + nx) * jl * mz + 8 * mx)
            hbm = pl.BlockSpec(memory_space=pltpu.HBM)
            block, grid, wx = pl.pallas_call(
                functools.partial(relay, (n, comps, xl, ny, nz, jl, mz)),
                out_shape=(
                    pltpu.VMEM((comps, mx, jl, mz), f32),
                    pltpu.VMEM((comps, nx, jl, mz), f32),
                    pltpu.VMEM((BAND, mx), f32),
                ),
                in_specs=[hbm] * 7,
                out_specs=(vmem, vmem, vmem),
                scratch_shapes=[
                    pltpu.VMEM((pairs, lanes, ny), f32),
                    pltpu.VMEM(((ny + REACH) * pairs, lanes), f32),
                    f32_rows(PLANES, plane, jl + REACH),
                    f32_rows(PLANES, plane, cl + REACH),
                    *shared,
                    pltpu.SMEM((my,), jnp.int32),
                    pltpu.SMEM((BAND, my), f32),
                    pltpu.VMEM((1, mz), jnp.int32),
                    pltpu.VMEM((BAND, mz), f32),
                    pltpu.VMEM((BAND, mx), f32),
                    pltpu.SMEM((mx,), jnp.int32),
                    pltpu.SMEM((BAND, mx), f32),
                    semaphores(pairs),
                    semaphores(6),
                    *[pltpu.SemaphoreType.DMA] * 3,
                    *[semaphores(PLANES)] * 5,
                    pltpu.SemaphoreType.REGULAR((chips,)),
                    pltpu.SemaphoreType.REGULAR,
                ],
                compiler_params=pltpu.CompilerParams(
                    collective_id=0, has_side_effects=True, vmem_limit_bytes=limit
                ),
                name="relay",
            )(slab, offsets_y, coeffs_y, offsets_z.reshape(1, mz), coeffs_z, coeffs_x, offsets_x)
            held = lambda array: pltpu.with_memory_space_constraint(array, pltpu.VMEM)
            return pl.pallas_call(
                finish,
                out_shape=jax.ShapeDtypeStruct((comps, mx, jl, mz), f32),
                in_specs=[vmem, vmem, vmem, hbm],
                out_specs=hbm,
                scratch_shapes=[
                    pltpu.VMEM((comps, mx, jl, mz), f32),
                    pltpu.SMEM((mx,), jnp.int32),
                    pltpu.SMEM((BAND, mx), f32),
                    semaphores(comps, 2),
                    semaphores(comps, 2),
                    semaphores(2),
                ],
                compiler_params=pltpu.CompilerParams(vmem_limit_bytes=limit),
                name="finish",
            )(held(block), held(grid), held(wx), offsets_x)
        grid, wx = pl.pallas_call(
            functools.partial(exchange, (n, comps, xl, ny, nz, jl, mz)),
            out_shape=(
                pltpu.VMEM((comps, nx, jl, mz), f32),
                jax.ShapeDtypeStruct((BAND, mx), f32),
            ),
            in_specs=[vmem, smem, smem, vmem, vmem, vmem],
            out_specs=(vmem, vmem),
            scratch_shapes=[
                pltpu.VMEM((ny * pairs, lanes), f32),
                f32_rows(chips, wide),
                f32_rows(chips, narrow),
                *shared,
                *[semaphores(chips)] * 4,
            ],
            compiler_params=pltpu.CompilerParams(collective_id=0, has_side_effects=True),
            name="exchange",
        )(slab, offsets_y, coeffs_y, offsets_z.reshape(1, mz), coeffs_z, coeffs_x)
        steps = 8
        return pl.pallas_call(
            functools.partial(refine_x, steps),
            out_shape=jax.ShapeDtypeStruct((comps, mx, jl, mz), f32),
            in_specs=[smem, smem, vmem],
            out_specs=pl.BlockSpec(memory_space=pltpu.HBM),
            scratch_shapes=[
                pltpu.VMEM((comps, mx, jl, mz), f32),
                pltpu.SemaphoreType.DMA((steps,)),
            ],
            name="refine_x",
        )(offsets_x, wx, pltpu.with_memory_space_constraint(grid, pltpu.VMEM))

    return jax.shard_map(
        body,
        mesh=mesh,
        in_specs=(P(None, "slab", None, None), P(), P(), P(), P(), P(), P()),
        out_specs=P(None, None, "slab", None),
        check_vma=False,
    )
```

```python
import functools

import jax
import jax.numpy as jnp
from jax import lax
from jax.experimental import pallas as pl
from jax.experimental.pallas import tpu as pltpu
from jax.sharding import PartitionSpec as P

MESH = pl.DeviceIdType.MESH
BAND = 4
REACH = BAND + 1
SPAN = BAND + 2
BELOW, ABOVE = 2, 3
PLANES = 4
GROUP = 8
VMEM_MOST = 67043328
LAST = (3, 2, 1, 1)


def flip(a, k, chips):
    out = 0
    bit = 1
    while bit < chips:
        a_bit, k_bit = lax.rem(lax.div(a, bit), 2), (k // bit) % 2
        out = out + (a_bit + k_bit - 2 * a_bit * k_bit) * bit
        bit *= 2
    return out


def span_of(me, jl, ny, j):
    return jnp.clip((me * jl + j) // 2 - 2, 0, ny - SPAN)


def make_weights(dims, me, span_base, oy_ref, cy_ref, oz_ref, cz_ref, cx_ref, wx_ref, wy, rz, rz_lo):
    n, comps, xl, ny, nz, jl, mz = dims
    pairs, lanes = wy.shape[1], wy.shape[2]
    fold = lanes // nz
    wx_ref[...] = cx_ref[...] / jnp.sum(cx_ref[...], axis=0, keepdims=True)
    wz = cz_ref[...] / jnp.sum(cz_ref[...], axis=0, keepdims=True)
    at = lax.broadcasted_iota(jnp.int32, (nz, mz), 0)
    first = jnp.broadcast_to(oz_ref[...], (nz, mz))
    band = jnp.zeros((nz, mz), jnp.float32)
    for k in range(BAND):
        band = band + jnp.where(at == first + k, jnp.broadcast_to(wz[k : k + 1], (nz, mz)), 0.0)
    high = band.astype(jnp.bfloat16)
    low = (band - high.astype(jnp.float32)).astype(jnp.bfloat16)
    rz[...] = jnp.zeros_like(rz)
    rz_lo[...] = jnp.zeros_like(rz_lo)
    for f in range(fold):
        rz[f * nz : (f + 1) * nz, f * mz : (f + 1) * mz] = high
        rz[lanes + f * nz : lanes + (f + 1) * nz, f * mz : (f + 1) * mz] = high
        rz_lo[f * nz : (f + 1) * nz, f * mz : (f + 1) * mz] = low
    for j in range(jl):
        coeffs = [jnp.full((pairs, lanes), cy_ref[k, me * jl + j]) for k in range(BAND)]
        total = coeffs[0] + coeffs[1] + coeffs[2] + coeffs[3]
        coeffs = [c / total for c in coeffs]
        skip = jnp.full((pairs, lanes), oy_ref[me * jl + j] - span_base(j))
        for m in range(SPAN):
            weight = jnp.zeros((pairs, lanes), jnp.float32)
            for k in range(max(0, m - SPAN + BAND), min(BAND, m + 1)):
                weight = jnp.where(skip == m - k, coeffs[k], weight)
            wy[j * SPAN + m] = weight


def refine_y(jl, pairs, span_base, wy, mixed, place, load, base):
    for j in range(jl):
        row = span_base(j) - base
        acc = wy[j * SPAN] * load(row)
        for m in range(1, SPAN):
            acc = acc + wy[j * SPAN + m] * load(row + m)
        mixed[pl.ds(place * pairs * jl + j, pairs, stride=jl), :] = acc


def refine_z(dims, pairs, mixed, rz, rz_lo, grid_ref, devices):
    n, comps, xl, ny, nz, jl, mz = dims
    fold = mixed.shape[1] // nz
    rows = pairs * jl * len(devices)
    x = mixed[:rows]
    hi = x.astype(jnp.bfloat16)
    lo = (x - hi.astype(jnp.float32)).astype(jnp.bfloat16)
    both = jnp.concatenate([hi, lo], axis=1)
    res = jnp.dot(both, rz[...], preferred_element_type=jnp.float32)
    res = res + jnp.dot(hi, rz_lo[...], preferred_element_type=jnp.float32)
    per = pairs // comps
    for q, device in enumerate(devices):
        for p in range(pairs):
            for f in range(fold):
                spot = (p // per, device * xl + (p % per) * fold + f)
                top = (q * pairs + p) * jl
                grid_ref[spot] = res[top : top + jl, f * mz : (f + 1) * mz]


def exchange(
    dims,
    points_ref, oy_ref, cy_ref, oz_ref, cz_ref, cx_ref,
    grid_ref, wx_ref,
    send, direct, passed, wy, rz, rz_lo, mixed,
    send_sem, recv_sem, pass_send_sem, pass_recv_sem,
):
    n, comps, xl, ny, nz, jl, mz = dims
    chips = n // 2
    pairs, lanes = points_ref.shape[0], points_ref.shape[1]
    cl = jl // 2
    wide, narrow = 2 * cl + REACH, cl + REACH
    me = lax.axis_index("slab")
    chip, core = me // 2, me % 2
    partner = chip * 2 + 1 - core

    def wide_base(c):
        return jnp.clip(c * 2 * cl - 2, 0, ny - wide)

    def narrow_base(d):
        return jnp.clip(d * cl - 2, 0, ny - narrow)

    span_base = functools.partial(span_of, me, jl, ny)

    rows_of_y = send.reshape(ny, pairs, lanes)

    barrier = pltpu.get_barrier_semaphore()
    pl.semaphore_signal(barrier, inc=1, device_id=(partner,), device_id_type=MESH)

    @pl.loop(1, chips)
    def _(k):
        other = flip(chip, k, chips) * 2 + core
        pl.semaphore_signal(barrier, inc=1, device_id=(other,), device_id_type=MESH)

    for p in range(pairs):
        send[pl.ds(p, ny, stride=pairs), :] = points_ref[p].T

    pl.semaphore_wait(barrier, chips)

    def out_copy(k):
        target = flip(chip, k, chips)
        return pltpu.make_async_remote_copy(
            src_ref=rows_of_y.at[pl.ds(wide_base(target), wide)],
            dst_ref=direct.at[k],
            send_sem=send_sem.at[k],
            recv_sem=recv_sem.at[k],
            device_id=(target * 2 + core,),
            device_id_type=MESH,
        )

    def pass_copy(k):
        skip = narrow_base(partner) - wide_base(chip)
        return pltpu.make_async_remote_copy(
            src_ref=direct.at[k, pl.ds(skip, narrow)],
            dst_ref=passed.at[k],
            send_sem=pass_send_sem.at[k],
            recv_sem=pass_recv_sem.at[k],
            device_id=(partner,),
            device_id_type=MESH,
        )

    @pl.loop(1, chips)
    def _(k):
        out_copy(k).start()

    own = pl.ds(wide_base(chip), wide)
    stay = pltpu.make_async_copy(rows_of_y.at[own], direct.at[0], recv_sem.at[0])
    stay.start()

    make_weights(dims, me, span_base, oy_ref, cy_ref, oz_ref, cz_ref, cx_ref, wx_ref, wy, rz, rz_lo)

    def from_direct(place, k):
        refine_y(
            jl, pairs, span_base, wy, mixed, place,
            lambda row: direct[k, row],
            wide_base(chip),
        )
        return flip(chip, k, chips) * 2 + core

    def from_passed(place, k):
        refine_y(
            jl, pairs, span_base, wy, mixed, place,
            lambda row: passed[k, row],
            narrow_base(me),
        )
        return flip(chip, k, chips) * 2 + 1 - core

    stay.wait()
    pass_copy(0).start()
    refine_z(dims, pairs, mixed, rz, rz_lo, grid_ref, [from_direct(0, 0)])

    @pl.loop(1, chips)
    def _(k):
        out_copy(k).wait_recv()
        pass_copy(k).start()
        one = from_direct(0, k)
        pass_copy(k - 1).wait_recv()
        two = from_passed(1, k - 1)
        refine_z(dims, pairs, mixed, rz, rz_lo, grid_ref, [one, two])

    pass_copy(chips - 1).wait_recv()
    refine_z(dims, pairs, mixed, rz, rz_lo, grid_ref, [from_passed(0, chips - 1)])

    @pl.loop(1, chips)
    def _(k):
        out_copy(k).wait_send()

    @pl.loop(0, chips)
    def _(k):
        pass_copy(k).wait_send()


def relay(
    dims,
    points_hbm, oy_hbm, cy_hbm, oz_hbm, cz_hbm, cx_hbm, ox_hbm,
    block_ref, grid_ref, wx_ref,
    slab, send, direct, passed, wy, rz, rz_lo, mixed,
    oy_ref, cy_ref, oz_ref, cz_ref, cx_ref,
    ox_ref, wx_scalars,
    load_sem, small_sem, out_sem, hand_sem, pass_sem,
    whole_recv, low_recv, high_recv, middle_recv, pass_recv,
    flags, partner_flag,
):
    n, comps, xl, ny, nz, jl, mz = dims
    chips = n // 2
    plane = chips // PLANES
    pairs, lanes = slab.shape[0], slab.shape[1]
    own, half = jl, jl // 2
    wide, narrow = own + REACH, half + REACH
    whole, low, high = pl.ds(0, wide), pl.ds(0, REACH), pl.ds(own, REACH)
    middle = pl.ds(REACH, own - REACH)
    low_inside, high_inside = pl.ds(BELOW, ABOVE), pl.ds(own, BELOW)
    me = lax.axis_index("slab")
    chip, core = lax.div(me, 2), lax.rem(me, 2)
    partner = chip * 2 + 1 - core
    here, level = lax.rem(chip, plane), lax.div(chip, plane)
    rows_of_y = send.reshape(ny + REACH, pairs, lanes)
    any_rows = direct.reshape(PLANES * plane * wide, pairs, lanes)
    span_base = functools.partial(span_of, me, jl, ny)
    around = [flip(here, d, plane) for d in range(plane)]

    loads = [pltpu.make_async_copy(points_hbm.at[p], slab.at[p], load_sem.at[p]) for p in range(pairs)]
    for load in loads:
        load.start()

    barrier = pltpu.get_barrier_semaphore()

    def greet(semaphore, device):
        pl.semaphore_signal(semaphore, inc=1, device_id=(device,), device_id_type=MESH)

    def device_of(z, q):
        return (z * plane + q) * 2 + core

    side = [lax.rem(here, 2), lax.div(here, 2)]
    above = [None, side[0] == 0, side[1] == 0, side[0] + side[1] == 0]
    below = [None, side[0] == 1, side[1] == 1, side[0] + side[1] == 2]
    missing = [None, side[0] == 0, side[1] == 0, side[0] + side[1] < 2]

    @pl.when(core == 0)
    def _():
        greet(barrier, partner)

    for d in range(plane):
        def hail(d=d):
            @pl.loop(level + (d == 0), PLANES)
            def _(z):
                greet(barrier, device_of(z, around[d]))

        hail() if d == 0 else pl.when(above[d])(hail)

    smalls = [
        pltpu.make_async_copy(src, dst, small_sem.at[i])
        for i, (src, dst) in enumerate(
            [(oy_hbm, oy_ref), (cy_hbm, cy_ref), (oz_hbm, oz_ref), (cz_hbm, cz_ref), (cx_hbm, cx_ref), (ox_hbm, ox_ref)]
        )
    ]
    for small in smalls:
        small.start()

    @pl.when(me > 0)
    def _():
        pl.semaphore_wait(barrier, (level + 1) * (1 + side[0]) * (1 + side[1]) - 1 + core)

    for d in range(plane):
        def answer(d=d):
            @pl.loop(0, level + (d != 0))
            def _(z):
                greet(flags.at[chip], device_of(z, around[d]))

        answer() if d == 0 else pl.when(below[d])(answer)

    def introduce(za, qa, zb, qb):
        greet(flags.at[zb * plane + qb], device_of(za, qa))
        greet(flags.at[za * plane + qa], device_of(zb, qb))

    for q in range(1, plane):
        @pl.when(here == q)
        def _():
            if q == plane - 1:
                introduce(level, 1, level, 2)

            @pl.loop(0, level)
            def _(z):
                for low_q in range(plane):
                    for high_q in range(plane):
                        if low_q | high_q == q and high_q != q:
                            if low_q & ~high_q:
                                introduce(z, low_q, level, high_q)

    @pl.when(core == 1)
    def _():
        greet(partner_flag, partner)

    for edge in (pl.ds(0, BELOW), pl.ds(BELOW + ny, ABOVE)):
        rows_of_y[edge] = jnp.zeros((edge.size, pairs, lanes), jnp.float32)
    for load in loads:
        load.wait()
    for p in range(pairs):
        send[pl.ds(BELOW * pairs + p, ny, stride=pairs), :] = slab[p].T

    def remote(src, dst, send_sem, recv_sem, device):
        return pltpu.make_async_remote_copy(
            src_ref=src, dst_ref=dst, send_sem=send_sem, recv_sem=recv_sem,
            device_id=(device,), device_id_type=MESH,
        )

    def await_recv(ref, semaphore):
        remote(ref, ref, out_sem, semaphore, partner).wait_recv()

    def await_send(count, semaphore):
        rows = any_rows.at[pl.ds(0, count)]
        remote(rows, rows, semaphore, pass_recv.at[0], partner).wait_send()

    def put(z, q, rows, semaphores):
        remote(
            rows_of_y.at[pl.ds((z * plane + q) * own + rows.start, rows.size)],
            direct.at[level, here, rows], out_sem, semaphores.at[level],
            (z * plane + q) * 2 + core,
        ).start()

    lacking = [None, side[0] == 0, side[1] == 0, here < plane - 1]

    def pick(mine, z, i):
        if z < mine:
            q, unknown = i, lacking[i]
        else:
            q, unknown = around[i], True if z > mine else missing[i]

        def wait():
            pl.semaphore_wait(flags.at[z * plane + q], 1)

        if unknown is True:
            wait()
        elif unknown is not None:
            pl.when(unknown)(wait)
        return q

    def send_whole(mine, z, places):
        for i in places:
            put(z, pick(mine, z, i), whole, whole_recv)

    def send_ends(mine, z, places):
        for i in places:
            q = pick(mine, z, i)
            if z == 0:
                pl.when(q == 0)(functools.partial(put, z, q, low_inside, low_recv))
                pl.when(q > 0)(functools.partial(put, z, q, low, low_recv))
            else:
                put(z, q, low, low_recv)
            edge = high_inside if z == PLANES - 1 else high
            pl.when(q == plane - 1)(functools.partial(put, z, q, edge, high_recv))

    def send_middle(mine, z, places):
        for i in places if z < mine else places[::-1]:
            put(z, i if z < mine else around[i], middle, middle_recv)

    def pass_copy(z):
        return remote(
            direct.at[z, :, pl.ds((1 - core) * half, narrow)], passed.at[z],
            pass_sem, pass_recv.at[z], partner,
        )

    def refine(blocks, base, devices):
        for j in range(jl):
            row = span_base(j) - base
            sums = [None] * len(blocks)
            for m in range(SPAN):
                weight = wy[j * SPAN + m]
                for i, block in enumerate(blocks):
                    term = weight * block[row + m]
                    sums[i] = term if m == 0 else sums[i] + term
            for i, total in enumerate(sums):
                mixed[pl.ds(i * pairs * jl + j, pairs, stride=jl), :] = total
        refine_z(dims, pairs, mixed, rz, rz_lo, grid_ref, devices)

    def take_whole(z):
        await_recv(direct.at[z], whole_recv.at[z])
        pass_copy(z).start()

    def take_plane(z):
        await_recv(direct.at[z, pl.ds(0, plane - 1)], whole_recv.at[z])
        pass_copy(z).start()

    def take_low(z):
        @pl.when(chip > 0)
        def _():
            await_recv(direct.at[z, :, low], low_recv.at[z])

        @pl.when(chip == 0)
        def _():
            await_recv(direct.at[z, :, low_inside], low_recv.at[z])

        @pl.when(here > 0)
        def _():
            remote(
                direct.at[z, :, low], direct.at[z, :, high], hand_sem, high_recv.at[z], (chip - 1) * 2 + core
            ).start()

    def take_middle(z):
        @pl.when(chip < chips - 1)
        def _():
            await_recv(direct.at[z, :, high], high_recv.at[z])

        @pl.when(chip == chips - 1)
        def _():
            await_recv(direct.at[z, :, high_inside], high_recv.at[z])

        await_recv(direct.at[z, :, middle], middle_recv.at[z])
        pass_copy(z).start()

    def near(z):
        refine(
            [direct.at[z, q] for q in range(plane)], chip * own - BELOW,
            [(z * plane + q) * 2 + core for q in range(plane)],
        )

    def far(z):
        pass_copy(z).wait_recv()
        refine(
            [passed.at[z, q] for q in range(plane)], me * half - BELOW,
            [(z * plane + q) * 2 + 1 - core for q in range(plane)],
        )

    mx, nx = wx_ref.shape[1], n * xl

    def across(known, written):
        fresh = groups_in(known, mx, nx) - written
        written |= fresh
        for start, stop in runs(fresh):
            refine_rows(start, stop, ox_ref, wx_scalars, grid_ref, block_ref)

    acts = {
        "W": send_whole, "E": send_ends, "M": send_middle,
        "w": take_whole, "p": take_plane, "e": take_low, "m": take_middle, "n": near, "f": far,
    }
    sends = [
        ["W1:0", "W0:123", "E2", "E3", "W1:123", "M3", "M2"],
        ["W0", "W1:123", "E2", "E3", "M3", "M2"],
        ["W3:0", "E0:012", "E1:012", "W3:12", "E0:3", "E1:3", "W3:3", "W2:123", "M0", "M1"],
        ["E0:012", "E1:012", "E0:3", "E1:3", "W2", "W3:123", "M0", "M1"],
    ]
    takes = [
        ["p0", "n0", "e2", "f0", "w1", "n1", "e3", "f1", "x", "m2", "n2", "m3", "f2", "x", "n3", "f3"],
        ["p1", "n1", "e3", "f1", "w0", "n0", "e2", "f0", "x", "m3", "n3", "m2", "f3", "n2", "x", "f2"],
        ["p2", "n2", "e1", "f2", "e0", "w3", "n3", "f3", "x", "m0", "n0", "m1", "f0", "n1", "x", "f1"],
        ["p3", "n3", "w2", "n2", "f3", "e0", "f2", "x", "e1", "m0", "n0", "m1", "f0", "n1", "x", "f1"],
    ]

    for z, plan in enumerate(sends):

        @pl.when(level == z)
        def _():
            for step in plan:
                target, _, places = step[1:].partition(":")
                acts[step[0]](z, int(target), [int(i) for i in places] or list(range(plane)))

    direct[level, here] = rows_of_y[pl.ds(chip * own, wide)]

    @pl.when(core == 0)
    def _():
        pl.semaphore_wait(partner_flag, 1)

    for small in smalls:
        small.wait()
    make_weights(dims, me, span_base, oy_ref, cy_ref, oz_ref, cz_ref, cx_ref, wx_ref, wy, rz, rz_lo)
    scalars = pltpu.make_async_copy(wx_ref, wx_scalars, small_sem.at[0])
    scalars.start()

    for z, plan in enumerate(takes):

        @pl.when(level == z)
        def _():
            known, written = set(), set()
            for step in plan:
                if step == "x":
                    if not written:
                        scalars.wait()
                    across(known, written)
                else:
                    acts[step[0]](int(step[1]))
                    known |= {int(step[1])} if step[0] == "f" else set()
            assert written == groups_in(set(range(PLANES)) - {LAST[z]}, mx, nx)

    ends = 2 * (plane * own + REACH) + (2 * plane - 1) * wide

    @pl.when(lax.div(level, 2) == 0)
    def _():
        await_send(ends - ABOVE, out_sem)

    @pl.when(lax.div(level, 2) == 1)
    def _():
        await_send(ends - BELOW, out_sem)

    @pl.when(here > 0)
    def _():
        await_send(2 * plane * REACH, hand_sem)

    await_send(PLANES * plane * narrow, pass_sem)


def refine_x(steps, ox_ref, wx_ref, grid_ref, out_ref, block, sems):
    comps, mx = block.shape[0], block.shape[1]
    rows = mx // steps

    def put(s):
        part = pl.ds(pl.multiple_of(s * rows, rows), rows)
        return pltpu.make_async_copy(block.at[:, part], out_ref.at[:, part], sems.at[s])

    @pl.loop(0, steps)
    def _(s):
        @pl.loop(0, rows // GROUP)
        def _(g):
            done = []
            for q in range(GROUP):
                i = s * rows + g * GROUP + q
                first = ox_ref[i]
                weights = [wx_ref[k, i] for k in range(BAND)]
                for c in range(comps):
                    acc = weights[0] * grid_ref[c, first]
                    for k in range(1, BAND):
                        acc = acc + weights[k] * grid_ref[c, first + k]
                    done.append((c, i, acc))
            for c, i, acc in done:
                block[c, i] = acc

        put(s).start()

    @pl.loop(0, steps)
    def _(s):
        put(s).wait()


def groups_in(known, mx, nx):
    depth = nx // PLANES
    inside = set()
    for g in range(mx // GROUP):
        low = max(g * GROUP // 2 - BELOW, 0) // depth
        high = min((g * GROUP + GROUP - 1) // 2 + ABOVE, nx - 1) // depth
        if set(range(low, high + 1)) <= known:
            inside.add(g)
    return inside


def runs(groups):
    out = []
    for start in sorted(g for g in groups if g - 1 not in groups):
        stop = start
        while stop in groups:
            stop += 1
        out.append((start, stop))
    return out


def refine_rows(start, stop, ox_ref, wx_ref, grid_ref, block_ref):
    comps = block_ref.shape[0]

    @pl.loop(start, stop)
    def _(g):
        done = []
        for r in range(GROUP):
            i = g * GROUP + r
            first = ox_ref[i]
            weights = [wx_ref[k, i] for k in range(BAND)]
            for c in range(comps):
                acc = weights[0] * grid_ref[c, first]
                for k in range(1, BAND):
                    acc = acc + weights[k] * grid_ref[c, first + k]
                done.append((c, i, acc))
        for c, i, acc in done:
            block_ref[c, i] = acc


def finish(ready_ref, grid_ref, wx_hbm, ox_hbm, out_ref, late_ref, ox_ref, wx_ref, out_sem, late_sem, small_sem):
    comps, mx = ready_ref.shape[:2]
    nx = grid_ref.shape[1]
    level = lax.div(lax.axis_index("slab"), 2 * PLANES)
    smalls = [
        pltpu.make_async_copy(src, dst, small_sem.at[i])
        for i, (src, dst) in enumerate([(ox_hbm, ox_ref), (wx_hbm, wx_ref)])
    ]
    for small in smalls:
        small.start()

    def put(src, c, start, stop, sem):
        rows = pl.ds(start * GROUP, (stop - start) * GROUP)
        return pltpu.make_async_copy(src.at[c, rows], out_ref.at[c, rows], sem)

    for z in range(PLANES):

        @pl.when(level == z)
        def _():
            ready = groups_in(set(range(PLANES)) - {LAST[z]}, mx, nx)
            late = runs(set(range(mx // GROUP)) - ready)
            early = [
                put(ready_ref, c, start, stop, out_sem.at[c, i])
                for i, (start, stop) in enumerate(runs(ready))
                for c in range(comps)
            ]
            for copy in early:
                copy.start()
            for small in smalls:
                small.wait()
            rest = []
            for i, (start, stop) in enumerate(late):
                refine_rows(start, stop, ox_ref, wx_ref, grid_ref, late_ref)
                rest += [put(late_ref, c, start, stop, late_sem.at[c, i]) for c in range(comps)]
            for copy in rest:
                copy.start()
            for copy in early + rest:
                copy.wait()


def solution(mesh):
    n = mesh.shape["slab"]
    vmem = pl.BlockSpec(memory_space=pltpu.VMEM)
    smem = pl.BlockSpec(memory_space=pltpu.SMEM)

    def body(points, offsets_x, coeffs_x, offsets_y, coeffs_y, offsets_z, coeffs_z):
        comps, xl, ny, nz = points.shape
        nx = xl * n
        mx, my, mz = offsets_x.shape[0], offsets_y.shape[0], offsets_z.shape[0]
        jl = my // n
        fold = 128 // nz
        pairs = comps * xl // fold
        lanes = fold * nz
        chips = n // 2
        cl = jl // 2
        wide, narrow = 2 * cl + REACH, cl + REACH
        slab = jnp.transpose(points, (0, 1, 3, 2)).reshape(pairs, lanes, ny)
        f32, bf16 = jnp.float32, jnp.bfloat16
        f32_rows = lambda *shape: pltpu.VMEM((*shape, pairs, lanes), f32)
        shared = [
            pltpu.VMEM((jl * SPAN, pairs, lanes), f32),
            pltpu.VMEM((2 * lanes, fold * mz), bf16),
            pltpu.VMEM((lanes, fold * mz), bf16),
            pltpu.VMEM((4 * pairs * jl, lanes), f32),
        ]
        semaphores = lambda *shape: pltpu.SemaphoreType.DMA(shape)
        if jl > REACH and chips == PLANES * PLANES and my == 2 * ny and mx % (PLANES * GROUP) == 0:
            plane = chips // PLANES
            limit = VMEM_MOST - 4 * (comps * (mx + nx) * jl * mz + 8 * mx)
            hbm = pl.BlockSpec(memory_space=pltpu.HBM)
            block, grid, wx = pl.pallas_call(
                functools.partial(relay, (n, comps, xl, ny, nz, jl, mz)),
                out_shape=(
                    pltpu.VMEM((comps, mx, jl, mz), f32),
                    pltpu.VMEM((comps, nx, jl, mz), f32),
                    pltpu.VMEM((BAND, mx), f32),
                ),
                in_specs=[hbm] * 7,
                out_specs=(vmem, vmem, vmem),
                scratch_shapes=[
                    pltpu.VMEM((pairs, lanes, ny), f32),
                    pltpu.VMEM(((ny + REACH) * pairs, lanes), f32),
                    f32_rows(PLANES, plane, jl + REACH),
                    f32_rows(PLANES, plane, cl + REACH),
                    *shared,
                    pltpu.SMEM((my,), jnp.int32),
                    pltpu.SMEM((BAND, my), f32),
                    pltpu.VMEM((1, mz), jnp.int32),
                    pltpu.VMEM((BAND, mz), f32),
                    pltpu.VMEM((BAND, mx), f32),
                    pltpu.SMEM((mx,), jnp.int32),
                    pltpu.SMEM((BAND, mx), f32),
                    semaphores(pairs),
                    semaphores(6),
                    *[pltpu.SemaphoreType.DMA] * 3,
                    *[semaphores(PLANES)] * 5,
                    pltpu.SemaphoreType.REGULAR((chips,)),
                    pltpu.SemaphoreType.REGULAR,
                ],
                compiler_params=pltpu.CompilerParams(
                    collective_id=0, has_side_effects=True, vmem_limit_bytes=limit
                ),
                name="relay",
            )(slab, offsets_y, coeffs_y, offsets_z.reshape(1, mz), coeffs_z, coeffs_x, offsets_x)
            held = lambda array: pltpu.with_memory_space_constraint(array, pltpu.VMEM)
            return pl.pallas_call(
                finish,
                out_shape=jax.ShapeDtypeStruct((comps, mx, jl, mz), f32),
                in_specs=[vmem, vmem, vmem, hbm],
                out_specs=hbm,
                scratch_shapes=[
                    pltpu.VMEM((comps, mx, jl, mz), f32),
                    pltpu.SMEM((mx,), jnp.int32),
                    pltpu.SMEM((BAND, mx), f32),
                    semaphores(comps, 2),
                    semaphores(comps, 2),
                    semaphores(2),
                ],
                compiler_params=pltpu.CompilerParams(vmem_limit_bytes=limit),
                name="finish",
            )(held(block), held(grid), held(wx), offsets_x)
        grid, wx = pl.pallas_call(
            functools.partial(exchange, (n, comps, xl, ny, nz, jl, mz)),
            out_shape=(
                pltpu.VMEM((comps, nx, jl, mz), f32),
                jax.ShapeDtypeStruct((BAND, mx), f32),
            ),
            in_specs=[vmem, smem, smem, vmem, vmem, vmem],
            out_specs=(vmem, vmem),
            scratch_shapes=[
                pltpu.VMEM((ny * pairs, lanes), f32),
                f32_rows(chips, wide),
                f32_rows(chips, narrow),
                *shared,
                *[semaphores(chips)] * 4,
            ],
            compiler_params=pltpu.CompilerParams(collective_id=0, has_side_effects=True),
            name="exchange",
        )(slab, offsets_y, coeffs_y, offsets_z.reshape(1, mz), coeffs_z, coeffs_x)
        steps = 8
        return pl.pallas_call(
            functools.partial(refine_x, steps),
            out_shape=jax.ShapeDtypeStruct((comps, mx, jl, mz), f32),
            in_specs=[smem, smem, vmem],
            out_specs=pl.BlockSpec(memory_space=pltpu.HBM),
            scratch_shapes=[
                pltpu.VMEM((comps, mx, jl, mz), f32),
                pltpu.SemaphoreType.DMA((steps,)),
            ],
            name="refine_x",
        )(offsets_x, wx, pltpu.with_memory_space_constraint(grid, pltpu.VMEM))

    return jax.shard_map(
        body,
        mesh=mesh,
        in_specs=(P(None, "slab", None, None), P(), P(), P(), P(), P(), P()),
        out_specs=P(None, None, "slab", None),
        check_vma=False,
    )
```
